256 devices in a mesh: ctx: 32 (over z, y_hi, core), kvh: 8 (over x, y_lo).
Axes of the slice: x: 4, y: 4 (y_hi: 2, y_lo: 2; y = y_hi * 2 + y_lo), z: 8, core: 2. Of those that a mesh axis runs over, the one named last changes fastest.
Arguments:
- queries: bfloat16 [4096, 8192], P('ctx', 'kvh'), may hold values from -40 to 40
- cache_keys: bfloat16 [16384, 1024], P('ctx', 'kvh'), may hold values from -6 to 6
- cache_values: bfloat16 [16384, 1024], P('ctx', 'kvh'), may hold values from -6 to 6
- new_keys: bfloat16 [4096, 1024], P('ctx', 'kvh'), may hold values from -6 to 6
- new_values: bfloat16 [4096, 1024], P('ctx', 'kvh'), may hold values from -6 to 6
- cache_fill: int32 [32], replicated, may hold values from 1 to 512, 8192 in all
- span_pos: int32 [32], P('ctx'), may hold values from 0 to 511
- destination: int32 [32], replicated, may hold values from 0 to 31, each once
Outputs:
- attn_out: bfloat16 [4096, 8192], P(('ctx', 'kvh'))
- appended_keys: bfloat16 [4096, 1024], P('ctx', 'kvh')
- appended_values: bfloat16 [4096, 1024], P('ctx', 'kvh')
The draws below stay inside these ranges and needn't reach their ends.
Inputs may be any that keep to these rules, and one draw needn't show every extreme that they name: `cache_fill`: every shard has at least one live token; the counts sum to 8192. `destination`: each slot is named by exactly one span.
All inputs are finite; a program needn't handle non-finite values.
Results may differ from the reference program's by a relative error of at most 0.007.
Values may be sent and summed in bfloat16 or wider, within the bound.
A program may use at most 64 MiB of HBM per device.

```python
import math
import jax
import jax.numpy as jnp
import numpy as np
from jax import lax

HD = 128
GROUP = 8
SPAN = 128
HOPS = 8
CH_DEV = 1
SHARD = 512
KVH = 8
SPANS = 32
TOKENS = 4096
CTX_TOK = 16384
N_CTX = 32


def shared_keys(key):
    subkey = jax.random.fold_in(key, 7)
    drawn = jax.random.normal(subkey, (N_CTX * SHARD, KVH * HD), jnp.float32)
    return jnp.clip(drawn, -6.0, 6.0)


def draw_cache_keys(key, part):
    return shared_keys(key).astype(jnp.bfloat16)


def draw_queries(key, part):
    subkey = jax.random.fold_in(key, 13)
    drawn = jax.random.normal(subkey, (TOKENS, KVH * GROUP * HD), jnp.float32)
    return jnp.clip(drawn, -6.0, 6.0).astype(jnp.bfloat16)


def with_ends(result, rng, least, high):
    extent = result.shape
    spot = [jax.random.randint(jax.random.fold_in(rng, axis), (), 0, extent[axis]) for axis in range(len(extent))]
    result = result.at[tuple(spot)].set(least)
    longest = extent.index(max(extent))
    spot[longest] = (spot[longest] + 1) % extent[longest]
    return result.at[tuple(spot)].set(high)


def block_levels(stream_key, shape, cuts, smallest, largest):
    loudness, own = 1.0, jax.random.fold_in(stream_key, 6)
    for axis_at, shards_of in cuts:
        heights = jnp.exp(jax.random.uniform(jax.random.fold_in(own, axis_at), (shards_of,), jnp.float32, smallest / len(cuts), largest / len(cuts)))
        loudness = loudness * jnp.repeat(heights, shape[axis_at] // shards_of).reshape([-1 if axis == axis_at else 1 for axis in range(len(shape))])
    return loudness


def split_up(count, total, most, lean):
    portions = [(1 << 20) // math.isqrt(grade ** lean) + 1 for grade in range(2, count + 1)]
    spare, holding = total - most - (count - 1), [1] * (count - 1)
    while spare > 0:
        candidates = [i for i in range(count - 1) if holding[i] < most]
        whole, remaining = sum([portions[i] for i in candidates]), spare
        for i in candidates:
            more = min(most - holding[i], max(1, remaining * portions[i] // whole), spare)
            holding[i] = holding[i] + more
            spare = spare - more
    return np.array([most] + holding)


def ragged(key, amount, total, most, slope):
    if amount == 2:
        one = jax.random.randint(key, (), max(1, total - most), min(most, total - 1) + 1)
        return jnp.stack([one, total - one])
    sizes = jnp.asarray(split_up(amount, total, most, slope), jnp.int32)
    twos = (amount - 1) // 2
    giver, receiver = sizes[1:1 + 2 * twos:2], sizes[2:2 + 2 * twos:2]
    slack = jnp.minimum(giver - 1, most - receiver)
    moved = jax.random.randint(jax.random.fold_in(key, 1), (twos,), 0, 1 << 20) % (slack + 1)
    sizes = sizes.at[1:1 + 2 * twos:2].set(giver - moved).at[2:2 + 2 * twos:2].set(receiver + moved)
    return sizes[jax.random.permutation(jax.random.fold_in(key, 2), amount)]


def bell_draw(key, extent, deviation, limit, pieces=(), kind=jnp.bfloat16):
    result = deviation * jax.random.normal(key, extent, jnp.float32)
    if pieces:
        result = result * block_levels(key, extent, pieces, -0.22, 0.18)
    return jnp.clip(result, -limit, limit).astype(kind)


def setup_inputs(seed: int = 0) -> dict:
    splits = jax.random.split(jax.random.key(seed), 9)
    return {
        "queries": draw_queries(jax.random.fold_in(splits[8], 71), 0),
        "cache_keys": draw_cache_keys(jax.random.fold_in(splits[8], 71), 0),
        "cache_values": bell_draw(splits[2], (CTX_TOK, KVH * HD), 1.0, 6.0, ((0, 32), (1, 8))),
        "new_keys": bell_draw(splits[3], (TOKENS, KVH * HD), 1.0, 6.0, ((0, 32), (1, 8))),
        "new_values": bell_draw(splits[4], (TOKENS, KVH * HD), 1.0, 6.0, ((0, 32), (1, 8))),
        "cache_fill": ragged(splits[5], N_CTX, N_CTX * SHARD // 2, SHARD, 2).astype(jnp.int32),
        "span_pos": with_ends(jax.random.randint(splits[6], (SPANS,), 0, SHARD), jax.random.fold_in(splits[6], 1), 0, SHARD - 1).astype(jnp.int32),
        "destination": jax.random.permutation(splits[7], SPANS).astype(jnp.int32),
    }


masked_score = -1.0e30


def reference(queries, cache_keys, cache_values, new_keys, new_values, cache_fill, span_pos, destination):
    scaling = HD ** -0.5
    query_all = queries.reshape(SPANS, SPAN, KVH, GROUP, HD)
    keys_cache = cache_keys.reshape(N_CTX, SHARD, KVH, HD)
    values_cache = cache_values.reshape(N_CTX, SHARD, KVH, HD)
    keys_fresh = new_keys.reshape(SPANS, SPAN, KVH, HD)
    values_fresh = new_values.reshape(SPANS, SPAN, KVH, HD)
    within = jnp.arange(SPAN, dtype=jnp.int32)
    places = jnp.arange(SHARD, dtype=jnp.int32)
    hop_ids = jnp.arange(HOPS, dtype=jnp.int32)

    def one_span(span_index):
        anchor = span_index // CH_DEV
        shards = ((anchor - hop_ids) % N_CTX).astype(jnp.int32)
        key_rows = jnp.concatenate([keys_fresh[span_index], keys_cache[shards].reshape(HOPS * SHARD, KVH, HD)], axis=0).astype(jnp.float32)
        value_rows = jnp.concatenate([values_fresh[span_index], values_cache[shards].reshape(HOPS * SHARD, KVH, HD)], axis=0).astype(jnp.float32)
        own_mask = within[None, :] <= within[:, None]
        live = places[None, :] < cache_fill[shards][:, None]
        reach = (hop_ids[None, :, None] > 0) | (places[None, None, :] <= span_pos[span_index] + within[:, None, None])
        cache_mask = (live[None] & reach).reshape(SPAN, HOPS * SHARD)
        visible = jnp.concatenate([own_mask, cache_mask], axis=1)
        scores = jnp.einsum('rhgd,khd->rhgk', query_all[span_index].astype(jnp.float32), key_rows) * scaling
        scores = jnp.where(visible[:, None, None, :], scores, masked_score)
        running_max = jnp.max(scores, axis=3, keepdims=True)
        weights = jnp.where(visible[:, None, None, :], jnp.exp(scores - running_max), 0.0)
        denominator = jnp.sum(weights, axis=3)
        packed = lax.optimization_barrier(weights.astype(jnp.bfloat16)).astype(jnp.float32)
        accum = jnp.einsum('rhgk,khd->rhgd', packed, value_rows)
        return (accum / denominator[..., None]).astype(jnp.bfloat16).reshape(SPAN, KVH * GROUP * HD)

    attn_out = lax.map(one_span, jnp.arange(SPANS, dtype=jnp.int32)).reshape(TOKENS, KVH * GROUP * HD)
    appended_keys = jnp.zeros((SPANS, SPAN, KVH * HD), jnp.bfloat16).at[destination].set(new_keys.reshape(SPANS, SPAN, KVH * HD)).reshape(TOKENS, KVH * HD)
    appended_values = jnp.zeros((SPANS, SPAN, KVH * HD), jnp.bfloat16).at[destination].set(new_values.reshape(SPANS, SPAN, KVH * HD)).reshape(TOKENS, KVH * HD)
    return attn_out, appended_keys, appended_values
```

```python
import functools
import math

import jax
import jax.numpy as jnp
from jax import lax
from jax.experimental import pallas as pl
from jax.experimental.pallas import tpu as pltpu
from jax.sharding import PartitionSpec as P

MESH = pl.DeviceIdType.MESH
SPAN = 128
HD = 128
GROUP = 8
SHARD = 512
HALF = 256
LANES = 256
VROWS = 144
BF = jnp.bfloat16
F32 = jnp.float32

FIRST = (
    ((1, 0, 0, 1, 0, 1, 0), (1, 1, 0, 0, 0, 1, 0), (1, 0, 0, 0, 0, 0, 2), (1, 1, 0, 1, 0, 0, 2), (1, 0, 0, 1, 0, 0, 1), (1, 1, 0, 0, 0, 0, 1), (1, 0, 0, 0, 0, 1, 0), (1, 1, 0, 1, 0, 0, 1), (1, 0, 0, 1, 0, 0, 2), (1, 0, 0, 0, 0, 0, 1), (1, 1, 0, 0, 0, 0, 2)),
    ((1, 0, 1, 0, 0, 0, 3), (1, 0, 1, 1, 0, 1, 1), (1, 1, 1, 1, 0, 0, 3), (1, 1, 1, 0, 0, 0, 3), (1, 1, 1, 0, 0, 1, 1), (1, 0, 1, 1, 0, 0, 3), (1, 1, 1, 1, 0, 1, 1)),
    ((1, 1, 2, 1, 0, 1, 2), (1, 0, 2, 1, 0, 0, 3), (1, 1, 2, 1, 0, 0, 3), (1, 1, 2, 0, 0, 0, 3), (1, 0, 2, 0, 0, 1, 2), (1, 0, 2, 1, 0, 1, 2), (1, 0, 2, 0, 0, 0, 3), (1, 1, 2, 0, 0, 1, 2)),
    ((1, 0, 3, 1, 0, 1, 3), (1, 1, 3, 0, 0, 0, 1), (1, 0, 3, 0, 0, 1, 3), (1, 1, 3, 1, 0, 0, 1)),
)
SEQ = (
    (
        ((0, 0, 0, 1, 1), (1, 0, 0, 1, 1, 0, 1), (0, 1, 0, 0, 1), (1, 1, 0, 0, 1, 0, 1), (0, 0, 1, 1, 1), (0, 0, 0, 0, 1), (1, 0, 0, 0, 1, 0, 2), (1, 0, 0, 0, 1, 0, 1), (0, 1, 1, 0, 1), (0, 1, 2, 1, 1), (1, 1, 2, 1, 1, 1, 0), (1, 1, 2, 1, 1, 0, 1), (0, 1, 1, 1, 1), (0, 1, 1, 0, 2), (0, 1, 3, 0, 1), (0, 0, 2, 0, 1), (1, 0, 2, 0, 1, 0, 1), (1, 0, 2, 0, 1, 1, 0), (0, 1, 3, 1, 1), (0, 0, 3, 1, 1), (0, 1, 1, 1, 2), (0, 0, 2, 1, 1), (1, 0, 2, 1, 1, 0, 1), (1, 0, 2, 1, 1, 1, 0), (0, 0, 3, 0, 1)),
        ((0, 1, 2, 0, 1), (1, 1, 2, 0, 1, 0, 1)),
        ((0, 1, 2, 1, 2), (1, 1, 2, 1, 2, 0, 1), (0, 1, 3, 0, 2), (0, 1, 0, 1, 1), (1, 1, 0, 1, 1, 0, 1)),
        ((0, 0, 3, 1, 2), (0, 1, 3, 1, 2), (0, 0, 2, 0, 2), (1, 0, 2, 0, 2, 0, 1), (0, 1, 2, 0, 2), (1, 1, 2, 0, 2, 0, 1), (0, 0, 1, 0, 1)),
        ((0, 0, 2, 1, 2), (1, 0, 2, 1, 2, 0, 1)),
        ((0, 0, 3, 0, 2),),
        ((0, 0, 1, 0, 2), (0, 0, 1, 1, 2)),
    ),
    (
        ((0, 0, 0, 1, 0), (0, 1, 0, 0, 0), (0, 1, 0, 1, 0), (0, 0, 0, 0, 0)),
        ((0, 1, 3, 0, 0), (1, 1, 3, 0, 0, 1, 1), (0, 0, 1, 1, 1), (1, 0, 1, 1, 1, 0, 3), (1, 0, 1, 1, 1, 0, 0), (0, 1, 3, 1, 0), (1, 1, 3, 1, 0, 1, 1), (0, 1, 1, 0, 1), (1, 1, 1, 0, 1, 1, 0), (1, 1, 1, 0, 1, 0, 3), (1, 1, 1, 0, 1, 0, 0), (0, 0, 0, 1, 1), (0, 1, 1, 1, 1), (1, 1, 1, 1, 1, 0, 0), (1, 1, 1, 1, 1, 1, 0), (1, 1, 1, 1, 1, 0, 3), (0, 1, 0, 0, 1), (0, 1, 3, 0, 1), (1, 1, 3, 0, 1, 0, 3), (1, 1, 3, 0, 1, 1, 1), (1, 1, 3, 0, 1, 0, 0), (0, 1, 3, 1, 1), (1, 1, 3, 1, 1, 1, 1), (1, 1, 3, 1, 1, 0, 3), (1, 1, 3, 1, 1, 0, 0), (0, 0, 3, 1, 1), (1, 0, 3, 1, 1, 0, 0), (0, 0, 0, 0, 1), (0, 0, 3, 0, 1), (1, 0, 3, 0, 1, 1, 1), (1, 0, 3, 0, 1, 0, 0)),
        ((0, 1, 2, 1, 1), (0, 1, 3, 0, 2), (1, 1, 3, 0, 2, 0, 0), (0, 0, 2, 0, 1), (0, 0, 3, 1, 2), (1, 0, 3, 1, 2, 0, 0), (0, 0, 2, 1, 1), (0, 1, 3, 1, 2), (1, 1, 3, 1, 2, 0, 0), (1, 1, 3, 1, 2, 0, 2), (0, 0, 1, 0, 1), (1, 0, 1, 0, 1, 0, 0), (1, 0, 1, 0, 1, 1, 0)),
        ((0, 1, 2, 0, 1),),
        ((0, 0, 3, 0, 2), (1, 0, 3, 0, 2, 0, 0)),
        ((0, 1, 2, 1, 2), (0, 1, 0, 1, 1)),
        ((0, 0, 2, 0, 2), (0, 1, 2, 0, 2), (0, 0, 2, 1, 2)),
    ),
    (
        ((0, 1, 2, 1, 1), (1, 1, 2, 1, 1, 0, 0), (1, 1, 2, 1, 1, 0, 3), (0, 0, 0, 0, 0), (1, 0, 0, 0, 0, 0, 3), (0, 0, 2, 0, 1), (1, 0, 2, 0, 1, 0, 0), (1, 0, 2, 0, 1, 0, 3), (0, 0, 3, 1, 1), (0, 1, 0, 1, 0), (1, 1, 0, 1, 0, 1, 2), (1, 1, 0, 1, 0, 0, 3), (0, 0, 1, 0, 0), (0, 0, 2, 1, 1), (1, 0, 2, 1, 1, 0, 3), (1, 0, 2, 1, 1, 0, 0), (0, 0, 3, 0, 1), (0, 1, 2, 0, 1), (1, 1, 2, 0, 1, 0, 0), (1, 1, 2, 0, 1, 1, 2), (1, 1, 2, 0, 1, 0, 3)),
        ((0, 0, 0, 1, 0), (1, 0, 0, 1, 0, 1, 2), (1, 0, 0, 1, 0, 0, 3), (0, 1, 1, 1, 0), (0, 1, 0, 0, 0), (1, 1, 0, 0, 0, 1, 2), (1, 1, 0, 0, 0, 0, 3)),
        ((0, 1, 1, 0, 0), (0, 0, 3, 1, 2), (0, 0, 3, 0, 2), (0, 1, 0, 1, 1), (1, 1, 0, 1, 1, 0, 3), (1, 1, 0, 1, 1, 0, 0), (0, 0, 1, 0, 1), (0, 0, 1, 1, 0)),
        ((0, 1, 2, 0, 2), (1, 1, 2, 0, 2, 0, 0), (0, 0, 1, 1, 1), (0, 0, 0, 1, 1), (1, 0, 0, 1, 1, 0, 3), (0, 0, 0, 0, 1), (1, 0, 0, 0, 1, 0, 3), (0, 1, 0, 0, 1), (1, 1, 0, 0, 1, 0, 3)),
        ((0, 1, 1, 0, 1), (0, 1, 1, 1, 1)),
        ((0, 1, 3, 0, 1), (0, 1, 3, 1, 1)),
        ((0, 1, 3, 0, 2), (0, 1, 3, 1, 2)),
    ),
    (
        ((0, 0, 2, 1, 0), (0, 1, 2, 1, 0), (0, 1, 2, 0, 0), (0, 0, 2, 0, 0)),
        ((0, 0, 3, 1, 1), (1, 0, 3, 1, 1, 1, 3), (1, 0, 3, 1, 1, 0, 2), (1, 0, 3, 1, 1, 0, 1), (0, 0, 1, 0, 0), (1, 0, 1, 0, 0, 1, 3), (1, 0, 1, 0, 0, 0, 2), (0, 0, 3, 0, 1), (1, 0, 3, 0, 1, 0, 2), (1, 0, 3, 0, 1, 1, 2), (1, 0, 3, 0, 1, 0, 1), (0, 1, 2, 1, 1), (0, 1, 1, 1, 0), (1, 1, 1, 1, 0, 0, 2), (0, 0, 0, 0, 0), (0, 0, 2, 0, 1), (0, 1, 1, 0, 0), (1, 1, 1, 0, 0, 0, 2), (0, 1, 0, 1, 0), (0, 0, 3, 1, 2), (1, 0, 3, 1, 2, 0, 1), (1, 0, 3, 1, 2, 0, 2), (0, 0, 2, 1, 1), (0, 0, 1, 0, 1), (1, 0, 1, 0, 1, 0, 1), (1, 0, 1, 0, 1, 0, 2), (0, 0, 1, 1, 0), (1, 0, 1, 1, 0, 0, 2)),
        ((0, 1, 2, 0, 1),),
        ((0, 0, 0, 1, 0), (0, 0, 1, 1, 1), (1, 0, 1, 1, 1, 1, 3), (1, 0, 1, 1, 1, 0, 2), (0, 1, 0, 0, 0)),
        ((0, 1, 1, 0, 1), (1, 1, 1, 0, 1, 0, 2), (0, 1, 0, 1, 1), (0, 1, 1, 1, 1), (1, 1, 1, 1, 1, 0, 2)),
        ((0, 1, 3, 0, 1), (1, 1, 3, 0, 1, 1, 2), (1, 1, 3, 0, 1, 0, 2), (0, 0, 1, 1, 2), (1, 0, 1, 1, 2, 0, 0), (0, 0, 0, 1, 1), (0, 0, 0, 0, 1), (0, 1, 3, 1, 1), (1, 1, 3, 1, 1, 0, 2)),
        ((0, 1, 0, 0, 1),),
    ),
)
ORDER = ((7, 6, 4, 5, 10, 11, 9), (0, 7, 5, 6, 11, 4, 10), (6, 0, 1, 4, 5, 7, 11), (2, 1, 6, 0, 5, 7, 4))
SPREAD = (1, 2, 3)


def slot_of(age, home):
    return age * 4 + home


def per_device(
    queries, cache_keys, cache_values, new_keys, new_values, cache_fill, span_pos, destination
):
    n_ctx = lax.axis_size("ctx")
    n_kvh = lax.axis_size("kvh")
    planes = n_ctx // 4
    pieces = n_ctx
    scaling = HD ** (-0.5) * math.log2(math.e)

    def kernel(
        q_ref, ck_ref, cv_ref, nk_ref, nv_ref, fill_ref, pos_ref, dest_ref,
        out_ref, ak_ref, av_ref,
        qt_ref, kb, vb, nvt, acc, m_ref, obuf, arecv, pk, w1, w2, app,
        ss, rs, a_s, a_r, w1s, w1r, w2s, w2r, spread,
    ):
        me = lax.axis_index("ctx")
        head = lax.axis_index("kvh")
        plane = me // 4
        role = lax.rem(me, 4)

        def at(up, r):
            return (lax.rem(plane + up + planes, planes) * 4 + r, head)

        barrier = pltpu.get_barrier_semaphore()
        near = [at(0, role ^ 1), at(0, role ^ 2), at(0, role ^ 3)]
        near += [at(1, role), at(-1, role), at(1, role ^ 1), at(-1, role ^ 1)]
        near += [(me, lax.rem(head + i, n_kvh)) for i in range(1, n_kvh)]
        for device in near:
            pl.semaphore_signal(barrier, inc=1, device_id=device, device_id_type=MESH)

        own = role
        live = fill_ref[me]
        keys = ck_ref[...].astype(F32)
        alive = lax.broadcasted_iota(jnp.int32, (SHARD, HD), 0) < live
        keys = jnp.where(alive, keys, keys[0:1, :]).astype(BF)
        values = jnp.where(alive, cv_ref[...].astype(F32), 0.0)
        for c in range(2):
            kb[own, c] = keys[c * HALF:(c + 1) * HALF]
            vb[own, c, 0:HD, :] = values[c * HALF:(c + 1) * HALF].T.astype(BF)
        for i in range(pieces // 2):
            pk[i] = nk_ref[i]
            pk[i + pieces // 2] = nv_ref[i]

        pl.semaphore_wait(barrier, len(near))

        sends = {}

        def piece(t, j, c, age):
            if t == 0:
                return kb.at[slot_of(age, j), c]
            return vb.at[slot_of(age, j), c, pl.ds(0, HD)]

        def remote(t, j, c, age, up, r, index):
            return pltpu.make_async_remote_copy(
                src_ref=piece(t, j, c, age),
                dst_ref=piece(t, j, c, age + up),
                send_sem=ss.at[index],
                recv_sem=rs.at[t, slot_of(age + up, j), c],
                device_id=at(up, r),
                device_id_type=MESH,
            )

        def act(r, action):
            if action[0] == 0:
                _, t, j, c, age = action
                pltpu.make_async_remote_copy(
                    src_ref=piece(t, j, c, age),
                    dst_ref=piece(t, j, c, age),
                    send_sem=ss.at[0],
                    recv_sem=rs.at[t, slot_of(age, j), c],
                    device_id=at(0, role ^ 1),
                    device_id_type=MESH,
                ).wait_recv()
            else:
                done = sends.setdefault(r, [])
                remote(*action[1:], len(done)).start()
                done.append(action[1:])

        for r in range(4):
            @pl.when(role == r)
            def _(r=r):
                for action in FIRST[r]:
                    act(r, action)

        def signal_planes(k, step):
            for up in (step, -step):
                pl.semaphore_signal(spread.at[k], inc=1, device_id=at(up, role), device_id_type=MESH)

        signal_planes(0, 1)

        for b in range(SPAN // 16):
            rows = [q_ref[b * 16:(b + 1) * 16, g * HD:(g + 1) * HD] for g in range(GROUP)]
            block = jnp.concatenate(rows, axis=0)
            qt_ref[:, b * 128:(b + 1) * 128] = block.astype(F32).T.astype(BF)
        row16 = lax.broadcasted_iota(jnp.int32, (16, HALF), 0)
        lane16 = lax.broadcasted_iota(jnp.int32, (16, HALF), 1)
        nvt[0:HD, :] = nv_ref[...].reshape(SPAN, HD).astype(F32).T.astype(BF)
        nvt[HD:VROWS, :] = jnp.where(row16[:, :SPAN] == 0, 1.0, 0.0).astype(BF)
        for age in range(3):
            for j in range(4):
                filled = fill_ref[at(-age, j)[0]]
                for c in range(2):
                    seen = (row16 == 0) & (lane16 + c * HALF < filled)
                    vb[slot_of(age, j), c, HD:VROWS, :] = jnp.where(seen, 1.0, 0.0).astype(BF)

        def tokens(tile, rows):
            lane = lax.broadcasted_iota(jnp.int32, (rows, LANES), 1)
            return (tile * 2 + lane // 128) * 16 + lane % 16

        def dot(a, b):
            return jnp.dot(a, b, preferred_element_type=F32)

        def lanes_of(tile):
            if isinstance(tile, int):
                return pl.ds(tile * LANES, LANES)
            return pl.ds(pl.multiple_of(tile * LANES, LANES), LANES)

        tiles = (GROUP * SPAN) // LANES

        for tile in range(tiles):
            lanes = lanes_of(tile)
            s = dot(nk_ref[...].reshape(SPAN, HD), qt_ref[:, lanes])
            row = lax.broadcasted_iota(jnp.int32, (SPAN, LANES), 0)
            s = jnp.where(row <= tokens(tile, SPAN), s, -1e30)
            top = jnp.max(s, axis=0, keepdims=True)
            weights = jnp.exp2((s - top) * scaling).astype(BF)
            acc[:, lanes] = dot(nvt[...], weights)
            m_ref[:, lanes] = top

        def attend(tile, slot, home):
            lanes = lanes_of(tile)
            qt = qt_ref[:, lanes]
            parts = []
            for c in range(2):
                s = dot(kb[slot, c], qt)
                if home:
                    row = lax.broadcasted_iota(jnp.int32, (HALF, LANES), 0) + c * HALF
                    s = jnp.where(row <= tokens(tile, HALF) + pos_ref[0], s, -1e30)
                parts.append(s)
            old = m_ref[:, lanes]
            top = jnp.maximum(old, jnp.max(jnp.maximum(parts[0], parts[1]), axis=0, keepdims=True))
            total = acc[:, lanes] * jnp.exp2((old - top) * scaling)
            for c in range(2):
                weights = jnp.exp2((parts[c] - top) * scaling).astype(BF)
                total = total + dot(vb[slot, c], weights)
            acc[:, lanes] = total
            m_ref[:, lanes] = top

        for tile in range(tiles):
            attend(tile, own, True)

        def spread_round(k):
            pl.semaphore_wait(spread.at[k], 2)
            if k == 0:
                signal_planes(1, 2)
            elif k == 1:
                signal_planes(2, 1)

        def stage_copy(src, dst, sems, semr, device, k, source):
            return pltpu.make_async_remote_copy(
                src_ref=src, dst_ref=dst, send_sem=sems.at[k], recv_sem=semr.at[source],
                device_id=(device, head), device_id_type=MESH,
            )

        def other(k):
            return lax.rem(me + k, n_ctx)

        def stage_one():
            w1[me] = pk[me]

            @pl.loop(1, n_ctx)
            def _(k):
                stage_copy(pk.at[other(k)], w1.at[me], w1s, w1r, other(k), k, me).start()

        def stage_two():
            @pl.loop(1, n_ctx)
            def _(k):
                d = other(k)
                stage_copy(pk.at[d], w1.at[d], w1s, w1r, d, k, d).wait()

            @pl.loop(0, n_ctx)
            def _(d):
                source = jnp.int32(0)
                for g in range(n_ctx):
                    source = jnp.maximum(source, jnp.where(dest_ref[g] == d, g, 0))
                w2[d] = w1[source]

            app[me] = w2[me]

            @pl.loop(1, n_ctx)
            def _(k):
                stage_copy(w2.at[other(k)], app.at[me], w2s, w2r, other(k), k, me).start()

        def communicate(step):
            for r in range(4):
                @pl.when(role == r)
                def _(r=r):
                    for i in range(7):
                        if SEQ[r][i]:
                            @pl.when(step == i)
                            def _(i=i):
                                for action in SEQ[r][i]:
                                    act(r, action)
            for k in range(3):
                @pl.when(step == SPREAD[k])
                def _(k=k):
                    spread_round(k)

            @pl.when(step == SPREAD[2])
            def _():
                stage_one()

            @pl.when(step == 6)
            def _():
                stage_two()

        def slot_at(step):
            slot = jnp.int32(0)
            for r in range(4):
                code = jnp.int32(ORDER[r][0])
                for i in range(1, 7):
                    code = jnp.where(step == i, ORDER[r][i], code)
                slot = jnp.where(role == r, code, slot)
            return slot

        @pl.loop(0, 6)
        def _(step):
            communicate(step)
            slot = slot_at(step)
            for tile in range(tiles):
                attend(tile, slot, False)

        communicate(6)
        last = slot_at(6)

        def out_copy(b):
            return pltpu.make_async_remote_copy(
                src_ref=obuf.at[b], dst_ref=arecv.at[head], send_sem=a_s.at[b], recv_sem=a_r.at[head],
                device_id=(me, b), device_id_type=MESH,
            )

        def ship(tile):
            for half in range(2):
                b = tile * 2 + half

                @pl.when(b != head)
                def _():
                    out_copy(b).start()

                @pl.when(b == head)
                def _():
                    arecv[b] = obuf[b]

        previous = None
        for i in range(tiles):
            tile = lax.rem(head // 2 + 1 + i, tiles)
            attend(tile, last, False)
            lanes = lanes_of(tile)
            result = acc[0:HD, lanes] * (1.0 / acc[HD:HD + 1, lanes])
            result = result.T.astype(BF)
            for half in range(2):
                for g in range(GROUP):
                    at_row = half * 128 + g * 16
                    obuf[tile * 2 + half, :, g * HD:(g + 1) * HD] = result[at_row:at_row + 16]
            if previous is not None:
                ship(previous)
            previous = tile
        ship(previous)

        for k in range(1, n_kvh):
            h = lax.rem(head + k, n_kvh)
            pltpu.make_async_remote_copy(
                src_ref=obuf.at[h], dst_ref=arecv.at[h], send_sem=a_s.at[h], recv_sem=a_r.at[h],
                device_id=(me, h), device_id_type=MESH,
            ).wait()
        for h in range(n_kvh):
            out_ref[:, h * GROUP * HD:(h + 1) * GROUP * HD] = arecv[h]

        @pl.loop(1, n_ctx)
        def _(k):
            d = other(k)
            stage_copy(w2.at[d], app.at[d], w2s, w2r, d, k, d).wait()

        for i in range(pieces // 2):
            ak_ref[i] = app[i]
            av_ref[i] = app[i + pieces // 2]

        for r in range(4):
            @pl.when(role == r)
            def _(r=r):
                for index, what in enumerate(sends[r]):
                    remote(*what, index).wait_send()

    half = pieces // 2
    rows8 = SPAN // half
    vmem = pl.BlockSpec(memory_space=pltpu.VMEM)
    smem = pl.BlockSpec(memory_space=pltpu.SMEM)
    dma = pltpu.SemaphoreType.DMA
    attn, keys, values = pl.pallas_call(
        kernel,
        out_shape=(
            jax.ShapeDtypeStruct((SPAN // n_kvh, n_kvh * GROUP * HD), BF),
            jax.ShapeDtypeStruct((half, rows8, HD), BF),
            jax.ShapeDtypeStruct((half, rows8, HD), BF),
        ),
        in_specs=[vmem] * 5 + [smem] * 3,
        out_specs=(vmem, vmem, vmem),
        scratch_shapes=[
            pltpu.VMEM((HD, GROUP * SPAN), BF),
            pltpu.VMEM((12, 2, HALF, HD), BF),
            pltpu.VMEM((12, 2, VROWS, HALF), BF),
            pltpu.VMEM((VROWS, SPAN), BF),
            pltpu.VMEM((VROWS, GROUP * SPAN), F32),
            pltpu.VMEM((1, GROUP * SPAN), F32),
            pltpu.VMEM((n_kvh, SPAN // n_kvh, GROUP * HD), BF),
            pltpu.VMEM((n_kvh, SPAN // n_kvh, GROUP * HD), BF),
            pltpu.VMEM((pieces, rows8, HD), BF),
            pltpu.VMEM((pieces, rows8, HD), BF),
            pltpu.VMEM((pieces, rows8, HD), BF),
            pltpu.VMEM((pieces, rows8, HD), BF),
            dma((48,)),
            dma((2, 12, 2)),
            dma((n_kvh,)),
            dma((n_kvh,)),
            dma((n_ctx,)),
            dma((n_ctx,)),
            dma((n_ctx,)),
            dma((n_ctx,)),
            pltpu.SemaphoreType.REGULAR((3,)),
        ],
        compiler_params=pltpu.CompilerParams(collective_id=0, has_side_effects=True),
        name="spanned_attention",
    )(
        queries, cache_keys, cache_values,
        new_keys.reshape(half, rows8, HD), new_values.reshape(half, rows8, HD),
        cache_fill, span_pos, destination,
    )
    return attn, keys.reshape(SPAN, HD), values.reshape(SPAN, HD)


def solution(mesh):
    placed = (
        P("ctx", "kvh"),
        P("ctx", "kvh"),
        P("ctx", "kvh"),
        P("ctx", "kvh"),
        P("ctx", "kvh"),
        P(),
        P("ctx"),
        P(),
    )
    return jax.shard_map(
        per_device,
        mesh=mesh,
        in_specs=placed,
        out_specs=(P(("ctx", "kvh"), None), P("ctx", "kvh"), P("ctx", "kvh")),
        check_vma=False,
    )
```

```python
import functools
import math

import jax
import jax.numpy as jnp
from jax import lax
from jax.experimental import pallas as pl
from jax.experimental.pallas import tpu as pltpu
from jax.sharding import PartitionSpec as P

MESH = pl.DeviceIdType.MESH
SPAN = 128
HD = 128
GROUP = 8
SHARD = 512
HALF = 256
LANES = 256
VROWS = 144
AHEAD = 4
BF = jnp.bfloat16
F32 = jnp.float32

FIRST = (
    ((1, 0, 0, 1, 0, 1, 0), (1, 1, 0, 0, 0, 1, 0), (1, 0, 0, 0, 0, 0, 2), (1, 1, 0, 1, 0, 0, 2), (1, 0, 0, 1, 0, 0, 1), (1, 1, 0, 0, 0, 0, 1), (1, 0, 0, 0, 0, 1, 0), (1, 1, 0, 1, 0, 0, 1), (1, 0, 0, 1, 0, 0, 2), (1, 0, 0, 0, 0, 0, 1), (1, 1, 0, 0, 0, 0, 2)),
    ((1, 0, 1, 0, 0, 0, 3), (1, 0, 1, 1, 0, 1, 1), (1, 1, 1, 1, 0, 0, 3), (1, 1, 1, 0, 0, 0, 3), (1, 1, 1, 0, 0, 1, 1), (1, 0, 1, 1, 0, 0, 3), (1, 1, 1, 1, 0, 1, 1)),
    ((1, 1, 2, 1, 0, 1, 2), (1, 0, 2, 1, 0, 0, 3), (1, 1, 2, 1, 0, 0, 3), (1, 1, 2, 0, 0, 0, 3), (1, 0, 2, 0, 0, 1, 2), (1, 0, 2, 1, 0, 1, 2), (1, 0, 2, 0, 0, 0, 3), (1, 1, 2, 0, 0, 1, 2)),
    ((1, 0, 3, 1, 0, 1, 3), (1, 1, 3, 0, 0, 0, 1), (1, 0, 3, 0, 0, 1, 3), (1, 1, 3, 1, 0, 0, 1)),
)
SEQ = (
    (
        ((2, 0), (0, 0, 0, 1, 1), (1, 0, 0, 1, 1, 0, 1), (0, 1, 0, 0, 1), (1, 1, 0, 0, 1, 0, 1), (0, 0, 1, 1, 1), (2, 1), (0, 0, 0, 0, 1), (1, 0, 0, 0, 1, 0, 2), (1, 0, 0, 0, 1, 0, 1), (0, 1, 1, 0, 1), (0, 1, 2, 1, 1), (1, 1, 2, 1, 1, 1, 0), (1, 1, 2, 1, 1, 0, 1), (0, 1, 1, 1, 1), (0, 1, 1, 0, 2), (0, 1, 3, 0, 1), (2, 2), (3,), (0, 0, 2, 0, 1), (1, 0, 2, 0, 1, 0, 1), (1, 0, 2, 0, 1, 1, 0), (0, 1, 3, 1, 1), (0, 0, 3, 1, 1), (0, 1, 1, 1, 2), (0, 0, 2, 1, 1), (1, 0, 2, 1, 1, 0, 1), (1, 0, 2, 1, 1, 1, 0), (0, 0, 3, 0, 1)),
        ((0, 1, 2, 0, 1), (1, 1, 2, 0, 1, 0, 1)),
        ((0, 1, 2, 1, 2), (1, 1, 2, 1, 2, 0, 1), (0, 1, 3, 0, 2), (0, 1, 0, 1, 1), (1, 1, 0, 1, 1, 0, 1)),
        ((0, 0, 3, 1, 2), (0, 1, 3, 1, 2), (0, 0, 2, 0, 2), (1, 0, 2, 0, 2, 0, 1), (0, 1, 2, 0, 2), (1, 1, 2, 0, 2, 0, 1), (0, 0, 1, 0, 1)),
        ((0, 0, 2, 1, 2), (1, 0, 2, 1, 2, 0, 1)),
        ((0, 0, 3, 0, 2),),
        ((0, 0, 1, 0, 2), (0, 0, 1, 1, 2)),
    ),
    (
        ((0, 0, 0, 1, 0), (0, 1, 0, 0, 0), (0, 1, 0, 1, 0), (0, 0, 0, 0, 0)),
        ((2, 0), (0, 1, 3, 0, 0), (1, 1, 3, 0, 0, 1, 1), (0, 0, 1, 1, 1), (1, 0, 1, 1, 1, 0, 3), (1, 0, 1, 1, 1, 0, 0), (0, 1, 3, 1, 0), (1, 1, 3, 1, 0, 1, 1), (0, 1, 1, 0, 1), (1, 1, 1, 0, 1, 1, 0), (1, 1, 1, 0, 1, 0, 3), (1, 1, 1, 0, 1, 0, 0), (0, 0, 0, 1, 1), (2, 1), (0, 1, 1, 1, 1), (1, 1, 1, 1, 1, 0, 0), (1, 1, 1, 1, 1, 1, 0), (1, 1, 1, 1, 1, 0, 3), (0, 1, 0, 0, 1), (0, 1, 3, 0, 1), (1, 1, 3, 0, 1, 0, 3), (1, 1, 3, 0, 1, 1, 1), (1, 1, 3, 0, 1, 0, 0), (0, 1, 3, 1, 1), (1, 1, 3, 1, 1, 1, 1), (1, 1, 3, 1, 1, 0, 3), (1, 1, 3, 1, 1, 0, 0), (0, 0, 3, 1, 1), (1, 0, 3, 1, 1, 0, 0), (0, 0, 0, 0, 1), (2, 2), (3,), (0, 0, 3, 0, 1), (1, 0, 3, 0, 1, 1, 1), (1, 0, 3, 0, 1, 0, 0)),
        ((0, 1, 2, 1, 1), (0, 1, 3, 0, 2), (1, 1, 3, 0, 2, 0, 0), (0, 0, 2, 0, 1), (0, 0, 3, 1, 2), (1, 0, 3, 1, 2, 0, 0), (0, 0, 2, 1, 1), (0, 1, 3, 1, 2), (1, 1, 3, 1, 2, 0, 0), (1, 1, 3, 1, 2, 0, 2), (0, 0, 1, 0, 1), (1, 0, 1, 0, 1, 0, 0), (1, 0, 1, 0, 1, 1, 0)),
        ((0, 1, 2, 0, 1),),
        ((0, 0, 3, 0, 2), (1, 0, 3, 0, 2, 0, 0)),
        ((0, 1, 2, 1, 2), (0, 1, 0, 1, 1)),
        ((0, 0, 2, 0, 2), (0, 1, 2, 0, 2), (0, 0, 2, 1, 2)),
    ),
    (
        ((2, 0), (0, 1, 2, 1, 1), (1, 1, 2, 1, 1, 0, 0), (1, 1, 2, 1, 1, 0, 3), (0, 0, 0, 0, 0), (1, 0, 0, 0, 0, 0, 3), (0, 0, 2, 0, 1), (1, 0, 2, 0, 1, 0, 0), (1, 0, 2, 0, 1, 0, 3), (0, 0, 3, 1, 1), (0, 1, 0, 1, 0), (1, 1, 0, 1, 0, 1, 2), (1, 1, 0, 1, 0, 0, 3), (0, 0, 1, 0, 0), (0, 0, 2, 1, 1), (1, 0, 2, 1, 1, 0, 3), (1, 0, 2, 1, 1, 0, 0), (2, 1), (0, 0, 3, 0, 1), (0, 1, 2, 0, 1), (1, 1, 2, 0, 1, 0, 0), (1, 1, 2, 0, 1, 1, 2), (1, 1, 2, 0, 1, 0, 3)),
        ((0, 0, 0, 1, 0), (1, 0, 0, 1, 0, 1, 2), (1, 0, 0, 1, 0, 0, 3), (0, 1, 1, 1, 0), (0, 1, 0, 0, 0), (1, 1, 0, 0, 0, 1, 2), (1, 1, 0, 0, 0, 0, 3)),
        ((0, 1, 1, 0, 0), (0, 0, 3, 1, 2), (2, 2), (3,), (0, 0, 3, 0, 2), (0, 1, 0, 1, 1), (1, 1, 0, 1, 1, 0, 3), (1, 1, 0, 1, 1, 0, 0), (0, 0, 1, 0, 1), (0, 0, 1, 1, 0)),
        ((0, 1, 2, 0, 2), (1, 1, 2, 0, 2, 0, 0), (0, 0, 1, 1, 1), (0, 0, 0, 1, 1), (1, 0, 0, 1, 1, 0, 3), (0, 0, 0, 0, 1), (1, 0, 0, 0, 1, 0, 3), (0, 1, 0, 0, 1), (1, 1, 0, 0, 1, 0, 3)),
        ((0, 1, 1, 0, 1), (0, 1, 1, 1, 1)),
        ((0, 1, 3, 0, 1), (0, 1, 3, 1, 1)),
        ((0, 1, 3, 0, 2), (0, 1, 3, 1, 2)),
    ),
    (
        ((0, 0, 2, 1, 0), (0, 1, 2, 1, 0), (0, 1, 2, 0, 0), (0, 0, 2, 0, 0)),
        ((2, 0), (0, 0, 3, 1, 1), (1, 0, 3, 1, 1, 1, 3), (1, 0, 3, 1, 1, 0, 2), (1, 0, 3, 1, 1, 0, 1), (0, 0, 1, 0, 0), (1, 0, 1, 0, 0, 1, 3), (1, 0, 1, 0, 0, 0, 2), (0, 0, 3, 0, 1), (1, 0, 3, 0, 1, 0, 2), (1, 0, 3, 0, 1, 1, 2), (1, 0, 3, 0, 1, 0, 1), (0, 1, 2, 1, 1), (0, 1, 1, 1, 0), (1, 1, 1, 1, 0, 0, 2), (0, 0, 0, 0, 0), (2, 1), (0, 0, 2, 0, 1), (0, 1, 1, 0, 0), (1, 1, 1, 0, 0, 0, 2), (0, 1, 0, 1, 0), (0, 0, 3, 1, 2), (1, 0, 3, 1, 2, 0, 1), (1, 0, 3, 1, 2, 0, 2), (0, 0, 2, 1, 1), (0, 0, 1, 0, 1), (1, 0, 1, 0, 1, 0, 1), (1, 0, 1, 0, 1, 0, 2), (0, 0, 1, 1, 0), (1, 0, 1, 1, 0, 0, 2)),
        ((0, 1, 2, 0, 1),),
        ((0, 0, 0, 1, 0), (2, 2), (3,), (0, 0, 1, 1, 1), (1, 0, 1, 1, 1, 1, 3), (1, 0, 1, 1, 1, 0, 2), (0, 1, 0, 0, 0)),
        ((0, 1, 1, 0, 1), (1, 1, 1, 0, 1, 0, 2), (0, 1, 0, 1, 1), (0, 1, 1, 1, 1), (1, 1, 1, 1, 1, 0, 2)),
        ((0, 1, 3, 0, 1), (1, 1, 3, 0, 1, 1, 2), (1, 1, 3, 0, 1, 0, 2), (0, 0, 1, 1, 2), (1, 0, 1, 1, 2, 0, 0), (0, 0, 0, 1, 1), (0, 0, 0, 0, 1), (0, 1, 3, 1, 1), (1, 1, 3, 1, 1, 0, 2)),
        ((0, 1, 0, 0, 1),),
    ),
)
STAGE_TWO = 5
ORDER = ((7, 6, 4, 5, 10, 11, 9), (0, 7, 5, 6, 11, 4, 10), (6, 0, 1, 4, 5, 7, 11), (2, 1, 6, 0, 5, 7, 4))


def slot_of(age, home):
    return age * 4 + home


def per_device(
    queries, cache_keys, cache_values, new_keys, new_values, cache_fill, span_pos, destination
):
    n_ctx = lax.axis_size("ctx")
    n_kvh = lax.axis_size("kvh")
    planes = n_ctx // 4
    pieces = n_ctx
    scaling = HD ** (-0.5) * math.log2(math.e)

    def kernel(
        q_hbm, ck_hbm, cv_hbm, nk_hbm, nv_hbm, fill_hbm, pos_hbm, dest_hbm,
        arecv, app,
        q_ref, ck_ref, cv_ref, fill_ref, pos_ref, dest_ref, inverse,
        qt_ref, kb, vb, nvt, acc, m_ref, obuf, pk, w1, w2,
        load, ss, rs, a_s, a_r, w1s, w1r, w2s, w2r, spread,
    ):
        me = lax.axis_index("ctx")
        head = lax.axis_index("kvh")
        plane = me // 4
        role = lax.rem(me, 4)

        def at(up, r):
            return (lax.rem(plane + up + planes, planes) * 4 + r, head)

        barrier = pltpu.get_barrier_semaphore()
        near = [at(0, role ^ 1), at(0, role ^ 2), at(0, role ^ 3)]
        near += [at(1, role), at(-1, role), at(1, role ^ 1), at(-1, role ^ 1)]
        near += [(me, lax.rem(head + i, n_kvh)) for i in range(1, n_kvh)]
        for device in near:
            pl.semaphore_signal(barrier, inc=1, device_id=device, device_id_type=MESH)

        half = pieces // 2
        loads = [
            pltpu.make_async_copy(src, dst, load.at[i])
            for i, (src, dst) in enumerate((
                (fill_hbm, fill_ref), (ck_hbm, ck_ref), (cv_hbm, cv_ref), (dest_hbm, dest_ref),
                (nk_hbm, pk.at[pl.ds(0, half)]), (nv_hbm, pk.at[pl.ds(half, half)]),
                (q_hbm, q_ref), (pos_hbm, pos_ref),
            ))
        ]
        for copy in loads:
            copy.start()
        for copy in loads[:4]:
            copy.wait()

        own = role
        live = fill_ref[me]
        keys = ck_ref[...].astype(F32)
        alive = lax.broadcasted_iota(jnp.int32, (SHARD, HD), 0) < live
        keys = jnp.where(alive, keys, keys[0:1, :]).astype(BF)
        values = jnp.where(alive, cv_ref[...].astype(F32), 0.0)
        for c in range(2):
            kb[own, c] = keys[c * HALF:(c + 1) * HALF]
            vb[own, c, 0:HD, :] = values[c * HALF:(c + 1) * HALF].T.astype(BF)

        @pl.loop(0, n_ctx)
        def _(d):
            source = jnp.int32(0)
            for g in range(n_ctx):
                source = jnp.maximum(source, jnp.where(dest_ref[g] == d, g, 0))
            inverse[d] = source

        for copy in loads[4:]:
            copy.wait()

        pl.semaphore_wait(barrier, len(near))

        sends = {}

        def piece(t, j, c, age):
            if t == 0:
                return kb.at[slot_of(age, j), c]
            return vb.at[slot_of(age, j), c, pl.ds(0, HD)]

        def remote(t, j, c, age, up, r, index):
            return pltpu.make_async_remote_copy(
                src_ref=piece(t, j, c, age),
                dst_ref=piece(t, j, c, age + up),
                send_sem=ss.at[index],
                recv_sem=rs.at[t, slot_of(age + up, j), c],
                device_id=at(up, r),
                device_id_type=MESH,
            )

        def act(r, action):
            if action[0] == 0:
                _, t, j, c, age = action
                pltpu.make_async_remote_copy(
                    src_ref=piece(t, j, c, age),
                    dst_ref=piece(t, j, c, age),
                    send_sem=ss.at[0],
                    recv_sem=rs.at[t, slot_of(age, j), c],
                    device_id=at(0, role ^ 1),
                    device_id_type=MESH,
                ).wait_recv()
            elif action[0] == 2:
                spread_round(action[1])
            elif action[0] == 3:
                stage_one()
            else:
                done = sends.setdefault(r, [])
                remote(*action[1:], len(done)).start()
                done.append(action[1:])

        for r in range(4):
            @pl.when(role == r)
            def _(r=r):
                for action in FIRST[r]:
                    act(r, action)

        def signal_planes(k, step):
            for up in (step, -step):
                pl.semaphore_signal(spread.at[k], inc=1, device_id=at(up, role), device_id_type=MESH)

        signal_planes(0, 1)

        for b in range(SPAN // 16):
            rows = [q_ref[b * 16:(b + 1) * 16, g * HD:(g + 1) * HD] for g in range(GROUP)]
            block = jnp.concatenate(rows, axis=0)
            qt_ref[:, b * 128:(b + 1) * 128] = block.astype(F32).T.astype(BF)
        row16 = lax.broadcasted_iota(jnp.int32, (16, HALF), 0)
        lane16 = lax.broadcasted_iota(jnp.int32, (16, HALF), 1)
        nvt[0:HD, :] = pk[half:pieces].reshape(SPAN, HD).astype(F32).T.astype(BF)
        nvt[HD:VROWS, :] = jnp.where(row16[:, :SPAN] == 0, 1.0, 0.0).astype(BF)
        for age in range(3):
            for j in range(4):
                filled = fill_ref[at(-age, j)[0]]
                for c in range(2):
                    seen = (row16 == 0) & (lane16 + c * HALF < filled)
                    vb[slot_of(age, j), c, HD:VROWS, :] = jnp.where(seen, 1.0, 0.0).astype(BF)

        def tokens(tile, rows):
            lane = lax.broadcasted_iota(jnp.int32, (rows, LANES), 1)
            return (tile * 2 + lane // 128) * 16 + lane % 16

        def dot(a, b):
            return jnp.dot(a, b, preferred_element_type=F32)

        def lanes_of(tile):
            if isinstance(tile, int):
                return pl.ds(tile * LANES, LANES)
            return pl.ds(pl.multiple_of(tile * LANES, LANES), LANES)

        tiles = (GROUP * SPAN) // LANES

        def own_scores(tile):
            s = dot(pk[0:half].reshape(SPAN, HD), qt_ref[:, lanes_of(tile)])
            row = lax.broadcasted_iota(jnp.int32, (SPAN, LANES), 0)
            return jnp.where(row <= tokens(tile, SPAN), s, -1e30)

        def own_absorb(tile, s):
            lanes = lanes_of(tile)
            top = jnp.max(s, axis=0, keepdims=True)
            weights = jnp.exp2((s - top) * scaling).astype(BF)
            acc[:, lanes] = dot(nvt[...], weights)
            m_ref[:, lanes] = top

        def shard_scores(slot, home, tile):
            qt = qt_ref[:, lanes_of(tile)]
            parts = []
            for c in range(2):
                s = dot(kb[slot, c], qt)
                if home:
                    row = lax.broadcasted_iota(jnp.int32, (HALF, LANES), 0) + c * HALF
                    s = jnp.where(row <= tokens(tile, HALF) + pos_ref[0], s, -1e30)
                parts.append(s)
            return parts

        def shard_absorb(slot, tile, parts):
            lanes = lanes_of(tile)
            old = m_ref[:, lanes]
            top = jnp.maximum(old, jnp.max(jnp.maximum(parts[0], parts[1]), axis=0, keepdims=True))
            total = acc[:, lanes] * jnp.exp2((old - top) * scaling)
            for c in range(2):
                weights = jnp.exp2((parts[c] - top) * scaling).astype(BF)
                total = total + dot(vb[slot, c], weights)
            acc[:, lanes] = total
            m_ref[:, lanes] = top

        def in_turn(order, scores, absorb, after=None):
            ahead = [scores(tile) for tile in order[:AHEAD]]
            for i, tile in enumerate(order):
                if i + AHEAD < len(order):
                    ahead.append(scores(order[i + AHEAD]))
                absorb(tile, ahead.pop(0))
                if after is not None:
                    after(i, tile)

        def attend(slot, home=False, order=tuple(range(tiles)), after=None):
            in_turn(
                order, functools.partial(shard_scores, slot, home), functools.partial(shard_absorb, slot), after
            )

        in_turn(tuple(range(tiles)), own_scores, own_absorb)
        attend(own, home=True)

        def spread_round(k):
            pl.semaphore_wait(spread.at[k], 2)
            if k == 0:
                signal_planes(1, 2)
            elif k == 1:
                signal_planes(2, 1)

        def stage_copy(src, dst, sems, semr, device, k, source):
            return pltpu.make_async_remote_copy(
                src_ref=src, dst_ref=dst, send_sem=sems.at[k], recv_sem=semr.at[source],
                device_id=(device, head), device_id_type=MESH,
            )

        def other(k):
            return lax.rem(me + k, n_ctx)

        def stage_one():
            w1[me] = pk[me]

            @pl.loop(1, n_ctx)
            def _(k):
                stage_copy(pk.at[other(k)], w1.at[me], w1s, w1r, other(k), k, me).start()

        def stage_two():
            @pl.loop(1, n_ctx)
            def _(k):
                d = other(k)
                stage_copy(pk.at[d], w1.at[d], w1s, w1r, d, k, d).wait()

            @pl.loop(0, n_ctx)
            def _(d):
                w2[d] = w1[inverse[d]]

            app[me] = w2[me]

            @pl.loop(1, n_ctx)
            def _(k):
                stage_copy(w2.at[other(k)], app.at[me], w2s, w2r, other(k), k, me).start()

        def communicate(step):
            for r in range(4):
                @pl.when(role == r)
                def _(r=r):
                    for i in range(7):
                        if SEQ[r][i]:
                            @pl.when(step == i)
                            def _(i=i):
                                for action in SEQ[r][i]:
                                    act(r, action)
            @pl.when(step == STAGE_TWO)
            def _():
                stage_two()

        def slot_at(step):
            slot = jnp.int32(0)
            for r in range(4):
                code = jnp.int32(ORDER[r][0])
                for i in range(1, 7):
                    code = jnp.where(step == i, ORDER[r][i], code)
                slot = jnp.where(role == r, code, slot)
            return slot

        @pl.loop(0, 6)
        def _(step):
            communicate(step)
            slot = slot_at(step)
            attend(slot)

        communicate(6)
        last = slot_at(6)

        def out_copy(b):
            return pltpu.make_async_remote_copy(
                src_ref=obuf.at[b], dst_ref=arecv.at[head], send_sem=a_s.at[b], recv_sem=a_r.at[head],
                device_id=(me, b), device_id_type=MESH,
            )

        def ship(tile):
            for half in range(2):
                b = tile * 2 + half

                @pl.when(b != head)
                def _():
                    out_copy(b).start()

                @pl.when(b == head)
                def _():
                    arecv[b] = obuf[b]

        turn = [lax.rem(head // 2 + 1 + i, tiles) for i in range(tiles)]

        def finish(i, tile):
            lanes = lanes_of(tile)
            result = acc[0:HD, lanes] * (1.0 / acc[HD:HD + 1, lanes])
            result = result.T.astype(BF)
            for part in range(2):
                for g in range(GROUP):
                    at_row = part * 128 + g * 16
                    obuf[tile * 2 + part, :, g * HD:(g + 1) * HD] = result[at_row:at_row + 16]
            if i > 0:
                ship(turn[i - 1])

        attend(last, order=turn, after=finish)
        ship(turn[-1])

        for k in range(1, n_kvh):
            h = lax.rem(head + k, n_kvh)
            pltpu.make_async_remote_copy(
                src_ref=obuf.at[h], dst_ref=arecv.at[h], send_sem=a_s.at[h], recv_sem=a_r.at[h],
                device_id=(me, h), device_id_type=MESH,
            ).wait()
        @pl.loop(1, n_ctx)
        def _(k):
            d = other(k)
            stage_copy(w2.at[d], app.at[d], w2s, w2r, d, k, d).wait()

        for r in range(4):
            @pl.when(role == r)
            def _(r=r):
                for index, what in enumerate(sends[r]):
                    remote(*what, index).wait_send()

    half = pieces // 2
    rows8 = SPAN // half
    vmem = pl.BlockSpec(memory_space=pltpu.VMEM)
    dma = pltpu.SemaphoreType.DMA
    blocks, spans = pl.pallas_call(
        kernel,
        out_shape=(
            jax.ShapeDtypeStruct((n_kvh, SPAN // n_kvh, GROUP * HD), BF),
            jax.ShapeDtypeStruct((pieces, rows8, HD), BF),
        ),
        in_specs=[pl.BlockSpec(memory_space=pl.ANY)] * 8,
        out_specs=(vmem, vmem),
        scratch_shapes=[
            pltpu.VMEM((SPAN, GROUP * HD), BF),
            pltpu.VMEM((SHARD, HD), BF),
            pltpu.VMEM((SHARD, HD), BF),
            pltpu.SMEM((n_ctx,), jnp.int32),
            pltpu.SMEM((1,), jnp.int32),
            pltpu.SMEM((n_ctx,), jnp.int32),
            pltpu.SMEM((n_ctx,), jnp.int32),
            pltpu.VMEM((HD, GROUP * SPAN), BF),
            pltpu.VMEM((12, 2, HALF, HD), BF),
            pltpu.VMEM((12, 2, VROWS, HALF), BF),
            pltpu.VMEM((VROWS, SPAN), BF),
            pltpu.VMEM((VROWS, GROUP * SPAN), F32),
            pltpu.VMEM((1, GROUP * SPAN), F32),
            pltpu.VMEM((n_kvh, SPAN // n_kvh, GROUP * HD), BF),
            pltpu.VMEM((pieces, rows8, HD), BF),
            pltpu.VMEM((pieces, rows8, HD), BF),
            pltpu.VMEM((pieces, rows8, HD), BF),
            dma((8,)),
            dma((48,)),
            dma((2, 12, 2)),
            dma((n_kvh,)),
            dma((n_kvh,)),
            dma((n_ctx,)),
            dma((n_ctx,)),
            dma((n_ctx,)),
            dma((n_ctx,)),
            pltpu.SemaphoreType.REGULAR((3,)),
        ],
        compiler_params=pltpu.CompilerParams(collective_id=0, has_side_effects=True),
        name="spanned_attention",
    )(
        queries, cache_keys, cache_values,
        new_keys.reshape(half, rows8, HD), new_values.reshape(half, rows8, HD),
        cache_fill, span_pos, destination,
    )

    def place(blocks_ref, spans_ref, out_ref, ak_ref, av_ref):
        for h in range(n_kvh):
            out_ref[:, h * GROUP * HD:(h + 1) * GROUP * HD] = blocks_ref[h]
        for i in range(half):
            ak_ref[i] = spans_ref[i]
            av_ref[i] = spans_ref[i + half]

    attn, keys, values = pl.pallas_call(
        place,
        out_shape=(
            jax.ShapeDtypeStruct((SPAN // n_kvh, n_kvh * GROUP * HD), BF),
            jax.ShapeDtypeStruct((half, rows8, HD), BF),
            jax.ShapeDtypeStruct((half, rows8, HD), BF),
        ),
        in_specs=[vmem] * 2,
        out_specs=(vmem,) * 3,
        name="place_outputs",
    )(blocks, spans)
    return attn, keys.reshape(SPAN, HD), values.reshape(SPAN, HD)


def solution(mesh):
    placed = (
        P("ctx", "kvh"),
        P("ctx", "kvh"),
        P("ctx", "kvh"),
        P("ctx", "kvh"),
        P("ctx", "kvh"),
        P(),
        P("ctx"),
        P(),
    )
    return jax.shard_map(
        per_device,
        mesh=mesh,
        in_specs=placed,
        out_specs=(P(("ctx", "kvh"), None), P("ctx", "kvh"), P("ctx", "kvh")),
        check_vma=False,
    )
```

```python
import functools
import math

import jax
import jax.numpy as jnp
from jax import lax
from jax.experimental import pallas as pl
from jax.experimental.pallas import tpu as pltpu
from jax.sharding import PartitionSpec as P

MESH = pl.DeviceIdType.MESH
SPAN = 128
HD = 128
GROUP = 8
SHARD = 512
HALF = 256
LANES = 256
VROWS = 144
AHEAD = 4
PAIR_AHEAD = 1
SINGLE = 3
BF = jnp.bfloat16
F32 = jnp.float32

FIRST = (
    ((1, 1, 0, 0, 0, 0, 3), (1, 0, 0, 0, 0, 1, 0), (1, 0, 0, 1, 0, 0, 3), (1, 1, 0, 0, 0, 0, 1), (1, 1, 0, 1, 0, 0, 2), (1, 1, 0, 0, 0, 1, 1), (1, 1, 0, 1, 0, 0, 1), (1, 0, 0, 1, 0, 1, 1), (1, 0, 0, 0, 0, 0, 2), (1, 0, 0, 0, 0, 0, 1), (1, 0, 0, 1, 0, 0, 1), (1, 1, 0, 1, 0, 1, 0)),
    ((1, 1, 1, 1, 0, 0, 3), (1, 1, 1, 0, 0, 1, 1), (1, 0, 1, 1, 0, 0, 3), (1, 0, 1, 0, 0, 0, 3), (1, 1, 1, 0, 0, 0, 3)),
    ((1, 1, 2, 0, 0, 1, 3), (1, 1, 2, 1, 0, 0, 3), (1, 0, 2, 1, 0, 0, 3), (1, 1, 2, 0, 0, 0, 3), (1, 1, 2, 1, 0, 1, 3), (1, 0, 2, 0, 0, 0, 3), (1, 0, 2, 1, 0, 1, 3), (1, 0, 2, 0, 0, 1, 3)),
    ((1, 0, 3, 1, 0, 0, 1), (1, 0, 3, 0, 0, 0, 1), (1, 1, 3, 0, 0, 1, 3), (1, 1, 3, 1, 0, 0, 1)),
)
SEQ = (
    (
        ((2, 0), (0, 0, 0, 0, 1), (1, 0, 0, 0, 1, 0, 2), (1, 0, 0, 0, 1, 0, 1), (5, 0), (2, 1), (0, 1, 0, 1, 1), (1, 1, 0, 1, 1, 0, 1), (0, 1, 0, 0, 1), (0, 0, 0, 1, 1)),
        ((0, 0, 3, 1, 1), (0, 1, 3, 0, 1), (0, 0, 3, 0, 1), (0, 1, 3, 1, 1)),
        ((0, 1, 2, 0, 1), (0, 1, 2, 1, 1), (2, 2), (3,), (5, 1), (0, 0, 2, 1, 1), (0, 0, 2, 0, 1)),
        ((0, 0, 3, 1, 2), (0, 0, 3, 0, 2), (0, 1, 3, 0, 2), (0, 1, 3, 1, 2)),
        ((0, 1, 1, 0, 1), (0, 1, 1, 1, 1), (0, 0, 1, 1, 1), (0, 0, 1, 0, 1)),
        ((0, 1, 2, 0, 2), (0, 1, 2, 1, 2), (0, 0, 2, 1, 2), (0, 0, 2, 0, 2)),
        ((0, 0, 1, 1, 2), (0, 1, 1, 1, 2), (0, 0, 1, 0, 2), (0, 1, 1, 0, 2)),
    ),
    (
        ((0, 1, 0, 0, 0), (0, 1, 0, 1, 0), (0, 0, 0, 0, 0), (0, 0, 0, 1, 0)),
        ((0, 1, 1, 0, 1), (1, 1, 1, 0, 1, 0, 3), (1, 1, 1, 0, 1, 0, 0), (0, 0, 3, 1, 0), (1, 0, 3, 1, 0, 1, 1), (2, 0), (0, 0, 3, 0, 0), (1, 0, 3, 0, 0, 1, 1), (0, 1, 0, 0, 1), (1, 1, 0, 0, 1, 0, 0), (1, 1, 0, 0, 1, 0, 3), (0, 1, 3, 1, 0), (1, 1, 3, 1, 0, 1, 1), (5, 0), (0, 0, 0, 1, 1), (1, 0, 0, 1, 1, 0, 0), (0, 0, 3, 1, 1), (1, 0, 3, 1, 1, 1, 1), (1, 0, 3, 1, 1, 0, 3), (1, 0, 3, 1, 1, 0, 0), (0, 1, 3, 0, 1), (1, 1, 3, 0, 1, 0, 0), (2, 1), (0, 0, 3, 0, 1), (1, 0, 3, 0, 1, 0, 3), (1, 0, 3, 0, 1, 1, 1), (1, 0, 3, 0, 1, 0, 0), (0, 1, 2, 0, 1), (1, 1, 2, 0, 1, 0, 0), (1, 1, 2, 0, 1, 1, 1), (0, 1, 3, 1, 1), (1, 1, 3, 1, 1, 1, 1), (1, 1, 3, 1, 1, 0, 3), (1, 1, 3, 1, 1, 0, 0), (0, 1, 2, 1, 1), (1, 1, 2, 1, 1, 0, 0), (1, 1, 2, 1, 1, 1, 1)),
        ((0, 0, 3, 1, 2), (1, 0, 3, 1, 2, 0, 2), (1, 0, 3, 1, 2, 0, 0), (0, 0, 2, 1, 1), (1, 0, 2, 1, 1, 1, 1), (1, 0, 2, 1, 1, 0, 0), (0, 0, 0, 0, 1), (0, 1, 0, 1, 1)),
        ((0, 0, 3, 0, 2), (1, 0, 3, 0, 2, 0, 0), (0, 1, 3, 0, 2), (1, 1, 3, 0, 2, 0, 0), (2, 2), (3,), (5, 1), (0, 1, 2, 0, 2), (1, 1, 2, 0, 2, 0, 0), (0, 0, 2, 0, 1), (1, 0, 2, 0, 1, 0, 0), (1, 0, 2, 0, 1, 1, 1)),
        ((0, 1, 3, 1, 2), (1, 1, 3, 1, 2, 0, 2), (1, 1, 3, 1, 2, 0, 0), (0, 1, 1, 1, 1), (1, 1, 1, 1, 1, 0, 0), (1, 1, 1, 1, 1, 1, 0)),
        ((0, 1, 2, 1, 2), (1, 1, 2, 1, 2, 0, 0), (0, 0, 1, 1, 1), (1, 0, 1, 1, 1, 0, 0), (0, 0, 2, 1, 2), (1, 0, 2, 1, 2, 0, 0), (0, 0, 1, 0, 1), (1, 0, 1, 0, 1, 0, 0), (1, 0, 1, 0, 1, 1, 0)),
        ((0, 0, 2, 0, 2), (1, 0, 2, 0, 2, 0, 0)),
    ),
    (
        ((2, 0), (5, 0), (2, 1), (0, 1, 0, 1, 0), (1, 1, 0, 1, 0, 0, 3), (1, 1, 0, 1, 0, 1, 2), (0, 1, 2, 0, 1), (0, 1, 2, 1, 1), (0, 0, 2, 1, 1), (0, 0, 2, 0, 1)),
        ((2, 2), (3,), (0, 0, 0, 0, 0), (1, 0, 0, 0, 0, 0, 3), (0, 1, 0, 0, 0), (0, 0, 0, 1, 0)),
        ((0, 1, 1, 1, 0), (0, 0, 1, 1, 0), (0, 0, 1, 0, 0), (5, 1), (0, 1, 1, 0, 0)),
        ((0, 0, 0, 0, 1), (1, 0, 0, 0, 1, 0, 3), (0, 1, 1, 1, 1), (0, 0, 1, 1, 1), (0, 0, 1, 0, 1), (0, 1, 1, 0, 1)),
        ((0, 1, 0, 1, 1), (1, 1, 0, 1, 1, 0, 3), (0, 0, 0, 1, 1), (0, 1, 0, 0, 1)),
        ((0, 1, 3, 0, 1), (0, 0, 3, 1, 1), (0, 0, 3, 0, 1), (0, 1, 3, 1, 1)),
        ((0, 1, 3, 0, 2), (0, 0, 3, 1, 2), (0, 0, 3, 0, 2), (0, 1, 3, 1, 2)),
    ),
    (
        ((0, 1, 2, 1, 0), (0, 0, 2, 1, 0), (0, 1, 2, 0, 0), (0, 0, 2, 0, 0)),
        ((0, 1, 3, 0, 1), (1, 1, 3, 0, 1, 1, 3), (1, 1, 3, 0, 1, 0, 1), (1, 1, 3, 0, 1, 0, 2), (2, 0), (0, 1, 2, 0, 1), (1, 1, 2, 0, 1, 0, 2), (1, 1, 2, 0, 1, 0, 1), (0, 1, 1, 1, 0), (1, 1, 1, 1, 0, 1, 3), (1, 1, 1, 1, 0, 0, 2), (0, 1, 2, 1, 1), (1, 1, 2, 1, 1, 0, 1), (1, 1, 2, 1, 1, 0, 2), (0, 1, 0, 0, 0), (1, 1, 0, 0, 0, 0, 2), (5, 0), (0, 0, 2, 1, 1), (1, 0, 2, 1, 1, 0, 1), (1, 0, 2, 1, 1, 0, 2), (0, 0, 1, 1, 0), (1, 0, 1, 1, 0, 1, 3), (1, 0, 1, 1, 0, 0, 2), (0, 0, 0, 1, 0), (1, 0, 0, 1, 0, 0, 2), (1, 0, 0, 1, 0, 1, 3), (0, 1, 3, 0, 2), (1, 1, 3, 0, 2, 0, 1), (1, 1, 3, 0, 2, 0, 2), (2, 1), (0, 0, 2, 0, 1), (1, 0, 2, 0, 1, 0, 1), (1, 0, 2, 0, 1, 0, 2), (0, 1, 1, 1, 1), (1, 1, 1, 1, 1, 0, 2), (1, 1, 1, 1, 1, 0, 1), (0, 0, 1, 0, 0), (1, 0, 1, 0, 0, 0, 2), (1, 0, 1, 0, 0, 1, 3)),
        ((0, 0, 1, 1, 1), (1, 0, 1, 1, 1, 0, 1), (1, 0, 1, 1, 1, 1, 3), (1, 0, 1, 1, 1, 0, 2), (0, 0, 0, 1, 1), (1, 0, 0, 1, 1, 0, 2), (0, 1, 1, 0, 0), (1, 1, 1, 0, 0, 0, 2)),
        ((0, 0, 1, 0, 1), (1, 0, 1, 0, 1, 0, 1), (1, 0, 1, 0, 1, 0, 2), (2, 2), (3,), (5, 1), (0, 1, 1, 0, 1), (1, 1, 1, 0, 1, 1, 3), (1, 1, 1, 0, 1, 0, 2)),
        ((0, 0, 1, 1, 2), (1, 0, 1, 1, 2, 0, 0), (0, 1, 0, 0, 1), (1, 1, 0, 0, 1, 0, 2), (0, 1, 0, 1, 0), (0, 0, 0, 0, 0)),
        ((0, 0, 3, 1, 1), (1, 0, 3, 1, 1, 0, 2), (0, 1, 1, 0, 2), (1, 1, 1, 0, 2, 0, 0), (0, 0, 3, 0, 1), (1, 0, 3, 0, 1, 0, 2), (1, 0, 3, 0, 1, 1, 2), (0, 1, 3, 1, 1), (1, 1, 3, 1, 1, 0, 2)),
        ((0, 0, 0, 0, 1), (0, 1, 0, 1, 1)),
    ),
)
STAGE_TWO = 5
ORDER = ((4, 7, 6, 11, 5, 10, 9), (0, 7, 4, 6, 11, 5, 10), (6, 0, 1, 5, 4, 7, 11), (2, 6, 1, 5, 0, 7, 4))


def slot_of(age, home):
    return age * 4 + home


def per_device(
    queries, cache_keys, cache_values, new_keys, new_values, cache_fill, span_pos, destination
):
    n_ctx = lax.axis_size("ctx")
    n_kvh = lax.axis_size("kvh")
    planes = n_ctx // 4
    pieces = n_ctx
    scaling = HD ** (-0.5) * math.log2(math.e)

    def kernel(
        q_hbm, ck_hbm, cv_hbm, nk_hbm, nv_hbm, fill_hbm, pos_hbm, dest_hbm,
        arecv, app,
        q_ref, ck_ref, cv_ref, fill_ref, pos_ref, dest_ref, inverse,
        qt_ref, kb, vb, nvt, acc, m_ref, obuf, pk, w1, w2,
        load, ss, rs, a_s, a_r, w_s, w_r, home, spread, across,
    ):
        me = lax.axis_index("ctx")
        head = lax.axis_index("kvh")
        plane = me // 4
        role = lax.rem(me, 4)

        def at(up, r):
            return (lax.rem(plane + up + planes, planes) * 4 + r, head)

        barrier = pltpu.get_barrier_semaphore()
        near = [at(0, role ^ 1), at(0, role ^ 2), at(0, role ^ 3)]
        near += [at(1, role), at(-1, role), at(1, role ^ 1), at(-1, role ^ 1)]
        beside = [(me, lax.rem(head + 2, n_kvh)), (me, lax.rem(head + n_kvh - 2, n_kvh)), (me, head ^ 1)]
        near += beside
        for device in near:
            pl.semaphore_signal(barrier, inc=1, device_id=device, device_id_type=MESH)

        half = pieces // 2
        loads = [
            pltpu.make_async_copy(src, dst, load.at[i])
            for i, (src, dst) in enumerate((
                (fill_hbm, fill_ref), (ck_hbm, ck_ref), (cv_hbm, cv_ref), (dest_hbm, dest_ref),
                (nk_hbm, pk.at[pl.ds(0, half)]), (nv_hbm, pk.at[pl.ds(half, half)]),
                (q_hbm, q_ref), (pos_hbm, pos_ref),
            ))
        ]
        for copy in loads:
            copy.start()
        for copy in loads[:3]:
            copy.wait()

        own = role
        live = fill_ref[me]
        keys = ck_ref[...].astype(F32)
        alive = lax.broadcasted_iota(jnp.int32, (SHARD, HD), 0) < live
        keys = jnp.where(alive, keys, keys[0:1, :]).astype(BF)
        values = jnp.where(alive, cv_ref[...].astype(F32), 0.0)
        for c in range(2):
            kb[own * 2 + c] = keys[c * HALF:(c + 1) * HALF]
            vb[own * 2 + c, 0:HD, :] = values[c * HALF:(c + 1) * HALF].T.astype(BF)

        for copy in loads[3:]:
            copy.wait()

        pl.semaphore_wait(barrier, len(near))

        def piece(t, j, c, age):
            if t == 0:
                return kb.at[slot_of(age, j) * 2 + c]
            return vb.at[slot_of(age, j) * 2 + c, pl.ds(0, HD)]

        def remote(t, j, c, age, up, r):
            return pltpu.make_async_remote_copy(
                src_ref=piece(t, j, c, age),
                dst_ref=piece(t, j, c, age + up),
                send_sem=ss.at[t],
                recv_sem=rs.at[t, slot_of(age + up, j), c],
                device_id=at(up, r),
                device_id_type=MESH,
            )

        def act(action):
            if action[0] == 0:
                _, t, j, c, age = action
                pltpu.make_async_remote_copy(
                    src_ref=piece(t, j, c, age),
                    dst_ref=piece(t, j, c, age),
                    send_sem=ss.at[t],
                    recv_sem=rs.at[t, slot_of(age, j), c],
                    device_id=at(0, role ^ 1),
                    device_id_type=MESH,
                ).wait_recv()
            elif action[0] == 2:
                spread_round(action[1])
            elif action[0] == 5:
                pl.semaphore_wait(across.at[action[1]], 3)
                if action[1] == 0:
                    signal_beside(1)
            elif action[0] == 3:
                stage_one()
            else:
                remote(*action[1:]).start()

        for r in range(4):
            @pl.when(role == r)
            def _(r=r):
                for action in FIRST[r]:
                    act(action)

        def signal_planes(k, step):
            for up in (step, -step):
                pl.semaphore_signal(spread.at[k], inc=1, device_id=at(up, role), device_id_type=MESH)

        def signal_beside(k):
            for device in beside:
                pl.semaphore_signal(across.at[k], inc=1, device_id=device, device_id_type=MESH)

        signal_planes(0, 1)
        signal_beside(0)

        @pl.loop(0, n_ctx)
        def _(d):
            source = jnp.int32(0)
            for g in range(n_ctx):
                source = jnp.maximum(source, jnp.where(dest_ref[g] == d, g, 0))
            inverse[d] = source

        for b in range(SPAN // 16):
            rows = [q_ref[b * 16:(b + 1) * 16, g * HD:(g + 1) * HD] for g in range(GROUP)]
            block = jnp.concatenate(rows, axis=0)
            qt_ref[:, b * 128:(b + 1) * 128] = block.astype(F32).T.astype(BF)
        row16 = lax.broadcasted_iota(jnp.int32, (16, HALF), 0)
        lane16 = lax.broadcasted_iota(jnp.int32, (16, HALF), 1)
        nvt[0:HD, :] = pk[half:pieces].reshape(SPAN, HD).astype(F32).T.astype(BF)
        nvt[HD:VROWS, :] = jnp.where(row16[:, :SPAN] == 0, 1.0, 0.0).astype(BF)
        for age in range(3):
            for j in range(4):
                filled = fill_ref[at(-age, j)[0]]
                for c in range(2):
                    seen = (row16 == 0) & (lane16 + c * HALF < filled)
                    vb[slot_of(age, j) * 2 + c, HD:VROWS, :] = jnp.where(seen, 1.0, 0.0).astype(BF)

        def tokens(tile, rows):
            lane = lax.broadcasted_iota(jnp.int32, (rows, LANES), 1)
            return (tile * 2 + lane // 128) * 16 + lane % 16

        def dot(a, b):
            return jnp.dot(a, b, preferred_element_type=F32)

        def lanes_of(tile):
            if isinstance(tile, int):
                return pl.ds(tile * LANES, LANES)
            return pl.ds(pl.multiple_of(tile * LANES, LANES), LANES)

        tiles = (GROUP * SPAN) // LANES

        def own_scores(tile):
            s = dot(pk[0:half].reshape(SPAN, HD), qt_ref[:, lanes_of(tile)])
            row = lax.broadcasted_iota(jnp.int32, (SPAN, LANES), 0)
            return jnp.where(row <= tokens(tile, SPAN), s, -1e30)

        def own_absorb(tile, s):
            lanes = lanes_of(tile)
            top = jnp.max(s, axis=0, keepdims=True)
            weights = jnp.exp2((s - top) * scaling).astype(BF)
            acc[:, lanes] = dot(nvt[...], weights)
            m_ref[:, lanes] = top

        def shard_scores(slots, home, tile):
            qt = qt_ref[:, lanes_of(tile)]
            parts = []
            for slot in slots:
                for c in range(2):
                    s = dot(kb[slot * 2 + c], qt)
                    if home:
                        row = lax.broadcasted_iota(jnp.int32, (HALF, LANES), 0) + c * HALF
                        s = jnp.where(row <= tokens(tile, HALF) + pos_ref[0], s, -1e30)
                    parts.append(s)
            return parts

        def shard_absorb(slots, tile, parts):
            lanes = lanes_of(tile)
            old = m_ref[:, lanes]
            top = jnp.maximum(old, jnp.max(functools.reduce(jnp.maximum, parts), axis=0, keepdims=True))
            total = acc[:, lanes] * jnp.exp2((old - top) * scaling)
            for i, part in enumerate(parts):
                weights = jnp.exp2((part - top) * scaling).astype(BF)
                total = total + dot(vb[slots[i // 2] * 2 + i % 2], weights)
            acc[:, lanes] = total
            m_ref[:, lanes] = top

        def in_turn(order, scores, absorb, after=None, depth=AHEAD):
            ahead = [scores(tile) for tile in order[:depth]]
            for i, tile in enumerate(order):
                if i + depth < len(order):
                    ahead.append(scores(order[i + depth]))
                absorb(tile, ahead.pop(0))
                if after is not None:
                    after(i, tile)

        def attend(slots, home=False, order=tuple(range(tiles)), after=None):
            in_turn(
                order,
                functools.partial(shard_scores, slots, home),
                functools.partial(shard_absorb, slots),
                after,
                AHEAD if len(slots) == 1 else PAIR_AHEAD,
            )

        in_turn(tuple(range(tiles)), own_scores, own_absorb)
        attend((own,), home=True)

        def spread_round(k):
            pl.semaphore_wait(spread.at[k], 2)
            if k == 0:
                signal_planes(1, 2)
            elif k == 1:
                signal_planes(2, 1)

        def stage_copy(src, dst, stage, device):
            return pltpu.make_async_remote_copy(
                src_ref=src, dst_ref=dst, send_sem=w_s.at[stage], recv_sem=w_r.at[stage],
                device_id=(device, head), device_id_type=MESH,
            )

        def stage_wait(src, dst, stage):
            most = pl.ds(0, n_ctx - 1)
            stage_copy(src.at[most], dst.at[most], stage, me ^ 1).wait()

        def other(k):
            return lax.rem(me + k, n_ctx)

        def stage_one():
            w1[me] = pk[me]

            @pl.loop(1, n_ctx)
            def _(k):
                stage_copy(pk.at[other(k)], w1.at[me], 0, other(k)).start()

        def stage_two():
            stage_wait(pk, w1, 0)

            @pl.loop(0, n_ctx)
            def _(d):
                w2[d] = w1[inverse[d]]

            pltpu.make_async_copy(w2.at[me], app.at[me], home.at[1]).start()

            @pl.loop(1, n_ctx)
            def _(k):
                stage_copy(w2.at[other(k)], app.at[me], 1, other(k)).start()

        def communicate(step):
            for r in range(4):
                @pl.when(role == r)
                def _(r=r):
                    for i in range(7) if not isinstance(step, int) else (step,):
                        if not isinstance(step, int):
                            if i >= SINGLE:
                                continue

                            @pl.when(step == i)
                            def _(i=i):
                                for action in SEQ[r][i]:
                                    act(action)
                        else:
                            for action in SEQ[r][i]:
                                act(action)
            if isinstance(step, int) and step == STAGE_TWO:
                stage_two()

        def slot_at(step):
            slot = jnp.int32(0)
            for r in range(4):
                code = jnp.int32(ORDER[r][0])
                for i in range(1, 7):
                    code = jnp.where(step == i, ORDER[r][i], code)
                slot = jnp.where(role == r, code, slot)
            return slot

        @pl.loop(0, SINGLE)
        def _(step):
            communicate(step)
            attend((slot_at(step),))

        for step in range(SINGLE, 5, 2):
            communicate(step)
            communicate(step + 1)
            attend((slot_at(step), slot_at(step + 1)))

        communicate(5)
        communicate(6)
        last = (slot_at(5), slot_at(6))

        def out_copy(b):
            return pltpu.make_async_remote_copy(
                src_ref=obuf.at[b], dst_ref=arecv.at[head], send_sem=a_s.at[b], recv_sem=a_r.at[head],
                device_id=(me, b), device_id_type=MESH,
            )

        def ship(tile):
            for half in range(2):
                b = tile * 2 + half

                @pl.when(b != head)
                def _():
                    out_copy(b).start()

                @pl.when(b == head)
                def _():
                    pltpu.make_async_copy(obuf.at[b], arecv.at[b], home.at[0]).start()

        turn = [lax.rem(head // 2 + i, tiles) for i in (2, 1, 3, 0)]

        def finish(i, tile):
            lanes = lanes_of(tile)
            result = acc[0:HD, lanes] * (1.0 / acc[HD:HD + 1, lanes])
            result = result.T.astype(BF)
            for part in range(2):
                for g in range(GROUP):
                    at_row = part * 128 + g * 16
                    obuf[tile * 2 + part, :, g * HD:(g + 1) * HD] = result[at_row:at_row + 16]
            if i > 0:
                ship(turn[i - 1])

        attend(last, order=turn, after=finish)
        ship(turn[-1])
        if STAGE_TWO == 7:
            stage_two()

        for k in range(1, n_kvh):
            h = lax.rem(head + k, n_kvh)
            pltpu.make_async_remote_copy(
                src_ref=obuf.at[h], dst_ref=arecv.at[h], send_sem=a_s.at[h], recv_sem=a_r.at[h],
                device_id=(me, h), device_id_type=MESH,
            ).wait()
        stage_wait(w2, app, 1)
        pltpu.make_async_copy(obuf.at[head], arecv.at[head], home.at[0]).wait()
        pltpu.make_async_copy(w2.at[me], app.at[me], home.at[1]).wait()

        for r in range(4):
            @pl.when(role == r)
            def _(r=r):
                for t in range(2):
                    actions = FIRST[r] + sum(SEQ[r], ())
                    count = sum(a[:2] == (1, t) for a in actions)
                    whole = kb.at[pl.ds(0, count)] if t == 0 else vb.at[pl.ds(0, count), pl.ds(0, HD)]
                    pltpu.make_async_remote_copy(
                        src_ref=whole, dst_ref=whole, send_sem=ss.at[t], recv_sem=rs.at[0, 0, 0],
                        device_id=at(0, role ^ 1), device_id_type=MESH,
                    ).wait_send()

    half = pieces // 2
    rows8 = SPAN // half
    dma = pltpu.SemaphoreType.DMA
    blocks, spans = pl.pallas_call(
        kernel,
        out_shape=(
            jax.ShapeDtypeStruct((n_kvh, SPAN // n_kvh, GROUP * HD), BF),
            jax.ShapeDtypeStruct((pieces, rows8, HD), BF),
        ),
        in_specs=[pl.BlockSpec(memory_space=pl.ANY)] * 6
        + [pl.BlockSpec(memory_space=pltpu.HBM), pl.BlockSpec(memory_space=pl.ANY)],
        out_specs=(pl.BlockSpec(memory_space=pl.ANY),) * 2,
        scratch_shapes=[
            pltpu.VMEM((SPAN, GROUP * HD), BF),
            pltpu.VMEM((SHARD, HD), BF),
            pltpu.VMEM((SHARD, HD), BF),
            pltpu.SMEM((n_ctx,), jnp.int32),
            pltpu.SMEM((1,), jnp.int32),
            pltpu.SMEM((n_ctx,), jnp.int32),
            pltpu.SMEM((n_ctx,), jnp.int32),
            pltpu.VMEM((HD, GROUP * SPAN), BF),
            pltpu.VMEM((24, HALF, HD), BF),
            pltpu.VMEM((24, VROWS, HALF), BF),
            pltpu.VMEM((VROWS, SPAN), BF),
            pltpu.VMEM((VROWS, GROUP * SPAN), F32),
            pltpu.VMEM((1, GROUP * SPAN), F32),
            pltpu.VMEM((n_kvh, SPAN // n_kvh, GROUP * HD), BF),
            pltpu.VMEM((pieces, rows8, HD), BF),
            pltpu.VMEM((pieces, rows8, HD), BF),
            pltpu.VMEM((pieces, rows8, HD), BF),
            dma((8,)),
            dma((2,)),
            dma((2, 12, 2)),
            dma((n_kvh,)),
            dma((n_kvh,)),
            dma((2,)),
            dma((2,)),
            dma((2,)),
            pltpu.SemaphoreType.REGULAR((3,)),
            pltpu.SemaphoreType.REGULAR((2,)),
        ],
        compiler_params=pltpu.CompilerParams(
            collective_id=0, has_side_effects=True
        ),
        name="spanned_attention",
    )(
        queries, cache_keys, cache_values,
        new_keys.reshape(half, rows8, HD), new_values.reshape(half, rows8, HD),
        cache_fill, span_pos, destination,
    )

    def place(blocks_ref, spans_ref, out_ref, ak_ref, av_ref, rows, spans_here, taken, given):
        def columns(ref, h):
            return ref.at[:, pl.ds(h * GROUP * HD, GROUP * HD)]

        moves = [
            (blocks_ref.at[h], columns(rows, h), columns(rows, h), columns(out_ref, h)) for h in range(n_kvh)
        ]
        for part, target in ((0, ak_ref), (half, av_ref)):
            some = pl.ds(part, half)
            moves.append((spans_ref.at[some], spans_here.at[some], spans_here.at[some], target))
        takes = [pltpu.make_async_copy(m[0], m[1], taken.at[i]) for i, m in enumerate(moves)]
        gives = [pltpu.make_async_copy(m[2], m[3], given.at[i]) for i, m in enumerate(moves)]
        for copy in takes:
            copy.start()
        for take, give in zip(takes, gives):
            take.wait()
            give.start()
        for copy in gives:
            copy.wait()

    anywhere = pl.BlockSpec(memory_space=pl.ANY)
    attn, keys, values = pl.pallas_call(
        place,
        out_shape=(
            jax.ShapeDtypeStruct((SPAN // n_kvh, n_kvh * GROUP * HD), BF),
            jax.ShapeDtypeStruct((half, rows8, HD), BF),
            jax.ShapeDtypeStruct((half, rows8, HD), BF),
        ),
        in_specs=[anywhere] * 2,
        out_specs=(anywhere,) * 3,
        scratch_shapes=[
            pltpu.VMEM((SPAN // n_kvh, n_kvh * GROUP * HD), BF),
            pltpu.VMEM((pieces, rows8, HD), BF),
            dma((n_kvh + 2,)),
            dma((n_kvh + 2,)),
        ],
        name="place_outputs",
    )(blocks, spans)
    return attn, keys.reshape(SPAN, HD), values.reshape(SPAN, HD)


def solution(mesh):
    placed = (
        P("ctx", "kvh"),
        P("ctx", "kvh"),
        P("ctx", "kvh"),
        P("ctx", "kvh"),
        P("ctx", "kvh"),
        P(),
        P("ctx"),
        P(),
    )
    return jax.shard_map(
        per_device,
        mesh=mesh,
        in_specs=placed,
        out_specs=(P(("ctx", "kvh"), None), P("ctx", "kvh"), P("ctx", "kvh")),
        check_vma=False,
    )
```

```python
import functools
import math

import jax
import jax.numpy as jnp
from jax import lax
from jax.experimental import pallas as pl
from jax.experimental.pallas import tpu as pltpu
from jax.sharding import PartitionSpec as P

MESH = pl.DeviceIdType.MESH
SPAN = 128
HD = 128
GROUP = 8
SHARD = 512
HALF = 256
LANES = 256
VROWS = 144
AHEAD = 4
PAIR_AHEAD = 1
SINGLE = 3
BF = jnp.bfloat16
F32 = jnp.float32

FIRST = (
    ((1, 1, 0, 0, 0, 0, 3), (1, 0, 0, 0, 0, 1, 0), (1, 0, 0, 1, 0, 0, 3), (1, 1, 0, 0, 0, 0, 1), (1, 1, 0, 1, 0, 0, 2), (1, 1, 0, 0, 0, 1, 1), (1, 1, 0, 1, 0, 0, 1), (1, 0, 0, 1, 0, 1, 1), (1, 0, 0, 0, 0, 0, 2), (1, 0, 0, 0, 0, 0, 1), (1, 0, 0, 1, 0, 0, 1), (1, 1, 0, 1, 0, 1, 0)),
    ((1, 1, 1, 1, 0, 0, 3), (1, 1, 1, 0, 0, 1, 1), (1, 0, 1, 1, 0, 0, 3), (1, 0, 1, 0, 0, 0, 3), (1, 1, 1, 0, 0, 0, 3)),
    ((1, 1, 2, 0, 0, 1, 3), (1, 1, 2, 1, 0, 0, 3), (1, 0, 2, 1, 0, 0, 3), (1, 1, 2, 0, 0, 0, 3), (1, 1, 2, 1, 0, 1, 3), (1, 0, 2, 0, 0, 0, 3), (1, 0, 2, 1, 0, 1, 3), (1, 0, 2, 0, 0, 1, 3)),
    ((1, 0, 3, 1, 0, 0, 1), (1, 0, 3, 0, 0, 0, 1), (1, 1, 3, 0, 0, 1, 3), (1, 1, 3, 1, 0, 0, 1)),
)
SEQ = (
    (
        ((2, 0), (0, 0, 0, 0, 1), (1, 0, 0, 0, 1, 0, 2), (1, 0, 0, 0, 1, 0, 1), (2, 1), (5, 0), (2, 2), (3,), (0, 1, 0, 1, 1), (1, 1, 0, 1, 1, 0, 1), (0, 1, 0, 0, 1), (0, 0, 0, 1, 1)),
        ((0, 0, 3, 1, 1), (0, 1, 3, 0, 1), (0, 0, 3, 0, 1), (0, 1, 3, 1, 1)),
        ((0, 1, 2, 0, 1), (0, 1, 2, 1, 1), (5, 1), (0, 0, 2, 1, 1), (0, 0, 2, 0, 1)),
        ((0, 0, 3, 1, 2), (0, 0, 3, 0, 2), (0, 1, 3, 0, 2), (0, 1, 3, 1, 2)),
        ((0, 1, 1, 0, 1), (0, 1, 1, 1, 1), (0, 0, 1, 1, 1), (0, 0, 1, 0, 1)),
        ((0, 1, 2, 0, 2), (0, 1, 2, 1, 2), (0, 0, 2, 1, 2), (0, 0, 2, 0, 2)),
        ((0, 0, 1, 1, 2), (0, 1, 1, 1, 2), (0, 0, 1, 0, 2), (0, 1, 1, 0, 2)),
    ),
    (
        ((0, 1, 0, 0, 0), (0, 1, 0, 1, 0), (0, 0, 0, 0, 0), (0, 0, 0, 1, 0)),
        ((2, 0), (0, 1, 1, 0, 1), (1, 1, 1, 0, 1, 0, 3), (1, 1, 1, 0, 1, 0, 0), (0, 0, 3, 1, 0), (1, 0, 3, 1, 0, 1, 1), (0, 0, 3, 0, 0), (1, 0, 3, 0, 0, 1, 1), (0, 1, 0, 0, 1), (1, 1, 0, 0, 1, 0, 0), (1, 1, 0, 0, 1, 0, 3), (2, 1), (0, 1, 3, 1, 0), (1, 1, 3, 1, 0, 1, 1), (5, 0), (0, 0, 0, 1, 1), (1, 0, 0, 1, 1, 0, 0), (0, 0, 3, 1, 1), (1, 0, 3, 1, 1, 1, 1), (1, 0, 3, 1, 1, 0, 3), (1, 0, 3, 1, 1, 0, 0), (0, 1, 3, 0, 1), (1, 1, 3, 0, 1, 0, 0), (2, 2), (3,), (0, 0, 3, 0, 1), (1, 0, 3, 0, 1, 0, 3), (1, 0, 3, 0, 1, 1, 1), (1, 0, 3, 0, 1, 0, 0), (0, 1, 2, 0, 1), (1, 1, 2, 0, 1, 0, 0), (1, 1, 2, 0, 1, 1, 1), (0, 1, 3, 1, 1), (1, 1, 3, 1, 1, 1, 1), (1, 1, 3, 1, 1, 0, 3), (1, 1, 3, 1, 1, 0, 0), (0, 1, 2, 1, 1), (1, 1, 2, 1, 1, 0, 0), (1, 1, 2, 1, 1, 1, 1)),
        ((0, 0, 3, 1, 2), (1, 0, 3, 1, 2, 0, 2), (1, 0, 3, 1, 2, 0, 0), (0, 0, 2, 1, 1), (1, 0, 2, 1, 1, 1, 1), (1, 0, 2, 1, 1, 0, 0), (0, 0, 0, 0, 1), (0, 1, 0, 1, 1)),
        ((0, 0, 3, 0, 2), (1, 0, 3, 0, 2, 0, 0), (0, 1, 3, 0, 2), (1, 1, 3, 0, 2, 0, 0), (5, 1), (0, 1, 2, 0, 2), (1, 1, 2, 0, 2, 0, 0), (0, 0, 2, 0, 1), (1, 0, 2, 0, 1, 0, 0), (1, 0, 2, 0, 1, 1, 1)),
        ((0, 1, 3, 1, 2), (1, 1, 3, 1, 2, 0, 2), (1, 1, 3, 1, 2, 0, 0), (0, 1, 1, 1, 1), (1, 1, 1, 1, 1, 0, 0), (1, 1, 1, 1, 1, 1, 0)),
        ((0, 1, 2, 1, 2), (1, 1, 2, 1, 2, 0, 0), (0, 0, 1, 1, 1), (1, 0, 1, 1, 1, 0, 0), (0, 0, 2, 1, 2), (1, 0, 2, 1, 2, 0, 0), (0, 0, 1, 0, 1), (1, 0, 1, 0, 1, 0, 0), (1, 0, 1, 0, 1, 1, 0)),
        ((0, 0, 2, 0, 2), (1, 0, 2, 0, 2, 0, 0)),
    ),
    (
        ((2, 0), (2, 1), (5, 0), (2, 2), (3,), (0, 1, 0, 1, 0), (1, 1, 0, 1, 0, 0, 3), (1, 1, 0, 1, 0, 1, 2), (0, 1, 2, 0, 1), (0, 1, 2, 1, 1), (0, 0, 2, 1, 1), (0, 0, 2, 0, 1)),
        ((0, 0, 0, 0, 0), (1, 0, 0, 0, 0, 0, 3), (0, 1, 0, 0, 0), (0, 0, 0, 1, 0)),
        ((0, 1, 1, 1, 0), (0, 0, 1, 1, 0), (0, 0, 1, 0, 0), (5, 1), (0, 1, 1, 0, 0)),
        ((0, 0, 0, 0, 1), (1, 0, 0, 0, 1, 0, 3), (0, 1, 1, 1, 1), (0, 0, 1, 1, 1), (0, 0, 1, 0, 1), (0, 1, 1, 0, 1)),
        ((0, 1, 0, 1, 1), (1, 1, 0, 1, 1, 0, 3), (0, 0, 0, 1, 1), (0, 1, 0, 0, 1)),
        ((0, 1, 3, 0, 1), (0, 0, 3, 1, 1), (0, 0, 3, 0, 1), (0, 1, 3, 1, 1)),
        ((0, 1, 3, 0, 2), (0, 0, 3, 1, 2), (0, 0, 3, 0, 2), (0, 1, 3, 1, 2)),
    ),
    (
        ((0, 1, 2, 1, 0), (0, 0, 2, 1, 0), (0, 1, 2, 0, 0), (0, 0, 2, 0, 0)),
        ((2, 0), (0, 1, 3, 0, 1), (1, 1, 3, 0, 1, 1, 3), (1, 1, 3, 0, 1, 0, 1), (1, 1, 3, 0, 1, 0, 2), (0, 1, 2, 0, 1), (1, 1, 2, 0, 1, 0, 2), (1, 1, 2, 0, 1, 0, 1), (0, 1, 1, 1, 0), (1, 1, 1, 1, 0, 1, 3), (1, 1, 1, 1, 0, 0, 2), (0, 1, 2, 1, 1), (1, 1, 2, 1, 1, 0, 1), (1, 1, 2, 1, 1, 0, 2), (2, 1), (0, 1, 0, 0, 0), (1, 1, 0, 0, 0, 0, 2), (5, 0), (0, 0, 2, 1, 1), (1, 0, 2, 1, 1, 0, 1), (1, 0, 2, 1, 1, 0, 2), (0, 0, 1, 1, 0), (1, 0, 1, 1, 0, 1, 3), (1, 0, 1, 1, 0, 0, 2), (0, 0, 0, 1, 0), (1, 0, 0, 1, 0, 0, 2), (1, 0, 0, 1, 0, 1, 3), (0, 1, 3, 0, 2), (1, 1, 3, 0, 2, 0, 1), (1, 1, 3, 0, 2, 0, 2), (2, 2), (3,), (0, 0, 2, 0, 1), (1, 0, 2, 0, 1, 0, 1), (1, 0, 2, 0, 1, 0, 2), (0, 1, 1, 1, 1), (1, 1, 1, 1, 1, 0, 2), (1, 1, 1, 1, 1, 0, 1), (0, 0, 1, 0, 0), (1, 0, 1, 0, 0, 0, 2), (1, 0, 1, 0, 0, 1, 3)),
        ((0, 0, 1, 1, 1), (1, 0, 1, 1, 1, 0, 1), (1, 0, 1, 1, 1, 1, 3), (1, 0, 1, 1, 1, 0, 2), (0, 0, 0, 1, 1), (1, 0, 0, 1, 1, 0, 2), (0, 1, 1, 0, 0), (1, 1, 1, 0, 0, 0, 2)),
        ((0, 0, 1, 0, 1), (1, 0, 1, 0, 1, 0, 1), (1, 0, 1, 0, 1, 0, 2), (5, 1), (0, 1, 1, 0, 1), (1, 1, 1, 0, 1, 1, 3), (1, 1, 1, 0, 1, 0, 2)),
        ((0, 0, 1, 1, 2), (1, 0, 1, 1, 2, 0, 0), (0, 1, 0, 0, 1), (1, 1, 0, 0, 1, 0, 2), (0, 1, 0, 1, 0), (0, 0, 0, 0, 0)),
        ((0, 0, 3, 1, 1), (1, 0, 3, 1, 1, 0, 2), (0, 1, 1, 0, 2), (1, 1, 1, 0, 2, 0, 0), (0, 0, 3, 0, 1), (1, 0, 3, 0, 1, 0, 2), (1, 0, 3, 0, 1, 1, 2), (0, 1, 3, 1, 1), (1, 1, 3, 1, 1, 0, 2)),
        ((0, 0, 0, 0, 1), (0, 1, 0, 1, 1)),
    ),
)
STAGE_TWO = 5
ORDER = ((4, 7, 6, 11, 5, 10, 9), (0, 7, 4, 6, 11, 5, 10), (6, 0, 1, 5, 4, 7, 11), (2, 6, 1, 5, 0, 7, 4))


def slot_of(age, home):
    return age * 4 + home


def per_device(
    queries, cache_keys, cache_values, new_keys, new_values, cache_fill, span_pos, destination
):
    n_ctx = lax.axis_size("ctx")
    n_kvh = lax.axis_size("kvh")
    planes = n_ctx // 4
    pieces = n_ctx
    scaling = HD ** (-0.5) * math.log2(math.e)

    def kernel(
        q_hbm, ck_hbm, cv_hbm, nk_hbm, nv_hbm, fill_hbm, pos_hbm, dest_hbm,
        arecv, app,
        q_ref, ck_ref, cv_ref, fill_ref, pos_ref, dest_ref, inverse,
        qt_ref, kb, vb, nvt, acc, m_ref, obuf, pk, w1, w2,
        load, ss, rs, a_s, a_r, w_s, w_r, home, spread, across,
    ):
        me = lax.axis_index("ctx")
        head = lax.axis_index("kvh")
        plane = me // 4
        role = lax.rem(me, 4)

        def at(up, r):
            return (lax.rem(plane + up + planes, planes) * 4 + r, head)

        barrier = pltpu.get_barrier_semaphore()
        near = [at(0, role ^ 1), at(0, role ^ 2), at(0, role ^ 3)]
        near += [at(1, role), at(-1, role), at(1, role ^ 1), at(-1, role ^ 1)]
        beside = [(me, lax.rem(head + 2, n_kvh)), (me, lax.rem(head + n_kvh - 2, n_kvh)), (me, head ^ 1)]
        near += beside
        for device in near:
            pl.semaphore_signal(barrier, inc=1, device_id=device, device_id_type=MESH)

        half = pieces // 2
        loads = [
            pltpu.make_async_copy(src, dst, load.at[i])
            for i, (src, dst) in enumerate((
                (fill_hbm, fill_ref), (ck_hbm, ck_ref), (cv_hbm, cv_ref), (dest_hbm, dest_ref),
                (nk_hbm, pk.at[pl.ds(0, half)]), (nv_hbm, pk.at[pl.ds(half, half)]),
                (q_hbm, q_ref), (pos_hbm, pos_ref),
            ))
        ]
        for copy in loads:
            copy.start()
        for copy in loads[:3]:
            copy.wait()

        own = role
        live = fill_ref[me]
        keys = ck_ref[...].astype(F32)
        alive = lax.broadcasted_iota(jnp.int32, (SHARD, HD), 0) < live
        keys = jnp.where(alive, keys, keys[0:1, :]).astype(BF)
        values = jnp.where(alive, cv_ref[...].astype(F32), 0.0)
        for c in range(2):
            kb[own * 2 + c] = keys[c * HALF:(c + 1) * HALF]
            vb[own * 2 + c, 0:HD, :] = values[c * HALF:(c + 1) * HALF].T.astype(BF)

        for copy in loads[3:]:
            copy.wait()

        pl.semaphore_wait(barrier, len(near))

        def piece(t, j, c, age):
            if t == 0:
                return kb.at[slot_of(age, j) * 2 + c]
            return vb.at[slot_of(age, j) * 2 + c, pl.ds(0, HD)]

        def remote(t, j, c, age, up, r):
            return pltpu.make_async_remote_copy(
                src_ref=piece(t, j, c, age),
                dst_ref=piece(t, j, c, age + up),
                send_sem=ss.at[t],
                recv_sem=rs.at[t, slot_of(age + up, j), c],
                device_id=at(up, r),
                device_id_type=MESH,
            )

        def act(action):
            if action[0] == 0:
                _, t, j, c, age = action
                pltpu.make_async_remote_copy(
                    src_ref=piece(t, j, c, age),
                    dst_ref=piece(t, j, c, age),
                    send_sem=ss.at[t],
                    recv_sem=rs.at[t, slot_of(age, j), c],
                    device_id=at(0, role ^ 1),
                    device_id_type=MESH,
                ).wait_recv()
            elif action[0] == 2:
                spread_round(action[1])
            elif action[0] == 5:
                pl.semaphore_wait(across.at[action[1]], 3)
                if action[1] == 0:
                    signal_beside(1)
            elif action[0] == 3:
                stage_one()
            else:
                remote(*action[1:]).start()

        for r in range(4):
            @pl.when(role == r)
            def _(r=r):
                for action in FIRST[r]:
                    act(action)

        def signal_planes(k, step):
            for up in (step, -step):
                pl.semaphore_signal(spread.at[k], inc=1, device_id=at(up, role), device_id_type=MESH)

        def signal_beside(k):
            for device in beside:
                pl.semaphore_signal(across.at[k], inc=1, device_id=device, device_id_type=MESH)

        signal_planes(0, 1)
        signal_beside(0)

        @pl.loop(0, n_ctx)
        def _(d):
            source = jnp.int32(0)
            for g in range(n_ctx):
                source = jnp.maximum(source, jnp.where(dest_ref[g] == d, g, 0))
            inverse[d] = source

        for b in range(SPAN // 16):
            rows = [q_ref[b * 16:(b + 1) * 16, g * HD:(g + 1) * HD] for g in range(GROUP)]
            block = jnp.concatenate(rows, axis=0)
            qt_ref[:, b * 128:(b + 1) * 128] = block.astype(F32).T.astype(BF)
        row16 = lax.broadcasted_iota(jnp.int32, (16, HALF), 0)
        lane16 = lax.broadcasted_iota(jnp.int32, (16, HALF), 1)
        nvt[0:HD, :] = pk[half:pieces].reshape(SPAN, HD).astype(F32).T.astype(BF)
        nvt[HD:VROWS, :] = jnp.where(row16[:, :SPAN] == 0, 1.0, 0.0).astype(BF)
        for age in range(3):
            for j in range(4):
                filled = fill_ref[at(-age, j)[0]]
                for c in range(2):
                    seen = (row16 == 0) & (lane16 + c * HALF < filled)
                    vb[slot_of(age, j) * 2 + c, HD:VROWS, :] = jnp.where(seen, 1.0, 0.0).astype(BF)

        def tokens(tile, rows):
            lane = lax.broadcasted_iota(jnp.int32, (rows, LANES), 1)
            return (tile * 2 + lane // 128) * 16 + lane % 16

        def dot(a, b):
            return jnp.dot(a, b, preferred_element_type=F32)

        def lanes_of(tile):
            if isinstance(tile, int):
                return pl.ds(tile * LANES, LANES)
            return pl.ds(pl.multiple_of(tile * LANES, LANES), LANES)

        tiles = (GROUP * SPAN) // LANES

        def own_scores(tile):
            s = dot(pk[0:half].reshape(SPAN, HD), qt_ref[:, lanes_of(tile)])
            row = lax.broadcasted_iota(jnp.int32, (SPAN, LANES), 0)
            return jnp.where(row <= tokens(tile, SPAN), s, -1e30)

        def own_absorb(tile, s):
            lanes = lanes_of(tile)
            top = jnp.max(s, axis=0, keepdims=True)
            weights = jnp.exp2((s - top) * scaling).astype(BF)
            acc[:, lanes] = dot(nvt[...], weights)
            m_ref[:, lanes] = top

        def shard_scores(slots, home, tile):
            qt = qt_ref[:, lanes_of(tile)]
            parts = []
            for slot in slots:
                for c in range(2):
                    s = dot(kb[slot * 2 + c], qt)
                    if home:
                        row = lax.broadcasted_iota(jnp.int32, (HALF, LANES), 0) + c * HALF
                        s = jnp.where(row <= tokens(tile, HALF) + pos_ref[0], s, -1e30)
                    parts.append(s)
            return parts

        def shard_absorb(slots, final, tile, parts):
            lanes = lanes_of(tile)
            old = m_ref[:, lanes]
            top = jnp.maximum(old, jnp.max(functools.reduce(jnp.maximum, parts), axis=0, keepdims=True))
            total = acc[:, lanes] * jnp.exp2((old - top) * scaling)
            for i, part in enumerate(parts):
                weights = jnp.exp2((part - top) * scaling).astype(BF)
                total = total + dot(vb[slots[i // 2] * 2 + i % 2], weights)
            if final:
                return total
            acc[:, lanes] = total
            m_ref[:, lanes] = top

        def in_turn(order, scores, absorb, after=None, depth=AHEAD):
            ahead = [scores(tile) for tile in order[:depth]]
            for i, tile in enumerate(order):
                if i + depth < len(order):
                    ahead.append(scores(order[i + depth]))
                total = absorb(tile, ahead.pop(0))
                if after is not None:
                    after(i, tile, total)

        def attend(slots, home=False, order=tuple(range(tiles)), after=None):
            in_turn(
                order,
                functools.partial(shard_scores, slots, home),
                functools.partial(shard_absorb, slots, after is not None),
                after,
                AHEAD if len(slots) == 1 else PAIR_AHEAD,
            )

        in_turn(tuple(range(tiles)), own_scores, own_absorb)
        attend((own,), home=True)

        def spread_round(k):
            pl.semaphore_wait(spread.at[k], 2)
            if k == 0:
                signal_planes(1, 2)
            elif k == 1:
                signal_planes(2, 1)

        def stage_copy(src, dst, stage, device):
            return pltpu.make_async_remote_copy(
                src_ref=src, dst_ref=dst, send_sem=w_s.at[stage], recv_sem=w_r.at[stage],
                device_id=(device, head), device_id_type=MESH,
            )

        def stage_wait(src, dst, stage):
            most = pl.ds(0, n_ctx - 1)
            stage_copy(src.at[most], dst.at[most], stage, me ^ 1).wait()

        def other(k):
            return lax.rem(me + k, n_ctx)

        def stage_one():
            w1[me] = pk[me]

            @pl.loop(1, n_ctx)
            def _(k):
                stage_copy(pk.at[other(k)], w1.at[me], 0, other(k)).start()

        def stage_two():
            stage_wait(pk, w1, 0)

            @pl.loop(0, n_ctx)
            def _(d):
                w2[d] = w1[inverse[d]]

            pltpu.make_async_copy(w2.at[me], app.at[me], home.at[1]).start()

            @pl.loop(1, n_ctx)
            def _(k):
                stage_copy(w2.at[other(k)], app.at[me], 1, other(k)).start()

        def communicate(step):
            for r in range(4):
                @pl.when(role == r)
                def _(r=r):
                    for i in range(7) if not isinstance(step, int) else (step,):
                        if not isinstance(step, int):
                            if i >= SINGLE:
                                continue

                            @pl.when(step == i)
                            def _(i=i):
                                for action in SEQ[r][i]:
                                    act(action)
                        else:
                            for action in SEQ[r][i]:
                                act(action)
            if isinstance(step, int) and step == STAGE_TWO:
                stage_two()

        def slot_at(step):
            slot = jnp.int32(0)
            for r in range(4):
                code = jnp.int32(ORDER[r][0])
                for i in range(1, 7):
                    code = jnp.where(step == i, ORDER[r][i], code)
                slot = jnp.where(role == r, code, slot)
            return slot

        @pl.loop(0, SINGLE)
        def _(step):
            communicate(step)
            attend((slot_at(step),))

        for step in range(SINGLE, 5, 2):
            communicate(step)
            communicate(step + 1)
            attend((slot_at(step), slot_at(step + 1)))

        communicate(5)
        communicate(6)
        last = (slot_at(5), slot_at(6))

        def out_copy(b):
            return pltpu.make_async_remote_copy(
                src_ref=obuf.at[b], dst_ref=arecv.at[head], send_sem=a_s.at[b], recv_sem=a_r.at[head],
                device_id=(me, b), device_id_type=MESH,
            )

        def ship(i):
            if i < tiles - 1:
                for part in range(2):
                    out_copy(turn[i] * 2 + part).start()
            else:
                out_copy(head ^ 1).start()
                pltpu.make_async_copy(obuf.at[head], arecv.at[head], home.at[0]).start()

        turn = [lax.rem(head // 2 + i, tiles) for i in (2, 1, 3, 0)]

        def finish(i, tile, total):
            result = total[0:HD] * (1.0 / total[HD:HD + 1])
            result = result.T.astype(BF)
            for part in range(2):
                for g in range(GROUP):
                    at_row = part * 128 + g * 16
                    obuf[tile * 2 + part, :, g * HD:(g + 1) * HD] = result[at_row:at_row + 16]
            if i > 0:
                ship(i - 1)

        attend(last, order=turn, after=finish)
        ship(tiles - 1)
        if STAGE_TWO == 7:
            stage_two()

        for k in range(1, n_kvh):
            h = lax.rem(head + k, n_kvh)
            pltpu.make_async_remote_copy(
                src_ref=obuf.at[h], dst_ref=arecv.at[h], send_sem=a_s.at[h], recv_sem=a_r.at[h],
                device_id=(me, h), device_id_type=MESH,
            ).wait()
        stage_wait(w2, app, 1)
        pltpu.make_async_copy(obuf.at[head], arecv.at[head], home.at[0]).wait()
        pltpu.make_async_copy(w2.at[me], app.at[me], home.at[1]).wait()

        for r in range(4):
            @pl.when(role == r)
            def _(r=r):
                for t in range(2):
                    actions = FIRST[r] + sum(SEQ[r], ())
                    count = sum(a[:2] == (1, t) for a in actions)
                    whole = kb.at[pl.ds(0, count)] if t == 0 else vb.at[pl.ds(0, count), pl.ds(0, HD)]
                    pltpu.make_async_remote_copy(
                        src_ref=whole, dst_ref=whole, send_sem=ss.at[t], recv_sem=rs.at[0, 0, 0],
                        device_id=at(0, role ^ 1), device_id_type=MESH,
                    ).wait_send()

    half = pieces // 2
    rows8 = SPAN // half
    dma = pltpu.SemaphoreType.DMA
    blocks, spans = pl.pallas_call(
        kernel,
        out_shape=(
            jax.ShapeDtypeStruct((n_kvh, SPAN // n_kvh, GROUP * HD), BF),
            jax.ShapeDtypeStruct((pieces, rows8, HD), BF),
        ),
        in_specs=[pl.BlockSpec(memory_space=pl.ANY)] * 6
        + [pl.BlockSpec(memory_space=pltpu.HBM), pl.BlockSpec(memory_space=pl.ANY)],
        out_specs=(pl.BlockSpec(memory_space=pl.ANY),) * 2,
        scratch_shapes=[
            pltpu.VMEM((SPAN, GROUP * HD), BF),
            pltpu.VMEM((SHARD, HD), BF),
            pltpu.VMEM((SHARD, HD), BF),
            pltpu.SMEM((n_ctx,), jnp.int32),
            pltpu.SMEM((1,), jnp.int32),
            pltpu.SMEM((n_ctx,), jnp.int32),
            pltpu.SMEM((n_ctx,), jnp.int32),
            pltpu.VMEM((HD, GROUP * SPAN), BF),
            pltpu.VMEM((32, HALF, HD), BF),
            pltpu.VMEM((32, VROWS, HALF), BF),
            pltpu.VMEM((VROWS, SPAN), BF),
            pltpu.VMEM((VROWS, GROUP * SPAN), F32),
            pltpu.VMEM((1, GROUP * SPAN), F32),
            pltpu.VMEM((n_kvh, SPAN // n_kvh, GROUP * HD), BF),
            pltpu.VMEM((pieces, rows8, HD), BF),
            pltpu.VMEM((pieces, rows8, HD), BF),
            pltpu.VMEM((pieces, rows8, HD), BF),
            dma((8,)),
            dma((2,)),
            dma((2, 12, 2)),
            dma((n_kvh,)),
            dma((n_kvh,)),
            dma((2,)),
            dma((2,)),
            dma((2,)),
            pltpu.SemaphoreType.REGULAR((3,)),
            pltpu.SemaphoreType.REGULAR((2,)),
        ],
        compiler_params=pltpu.CompilerParams(
            collective_id=0, has_side_effects=True
        ),
        name="spanned_attention",
    )(
        queries, cache_keys, cache_values,
        new_keys.reshape(half, rows8, HD), new_values.reshape(half, rows8, HD),
        cache_fill, span_pos, destination,
    )

    def place(blocks_ref, spans_ref, out_ref, ak_ref, av_ref, rows, spans_here, taken, given):
        def columns(ref, h):
            return ref.at[:, pl.ds(h * GROUP * HD, GROUP * HD)]

        moves = [
            (blocks_ref.at[h], columns(rows, h), columns(rows, h), columns(out_ref, h)) for h in range(n_kvh)
        ]
        for part, target in ((0, ak_ref), (half, av_ref)):
            some = pl.ds(part, half)
            moves.append((spans_ref.at[some], spans_here.at[some], spans_here.at[some], target))
        takes = [pltpu.make_async_copy(m[0], m[1], taken.at[i]) for i, m in enumerate(moves)]
        gives = [pltpu.make_async_copy(m[2], m[3], given.at[i]) for i, m in enumerate(moves)]
        for copy in takes:
            copy.start()
        for take, give in zip(takes, gives):
            take.wait()
            give.start()
        for copy in gives:
            copy.wait()

    anywhere = pl.BlockSpec(memory_space=pl.ANY)
    attn, keys, values = pl.pallas_call(
        place,
        out_shape=(
            jax.ShapeDtypeStruct((SPAN // n_kvh, n_kvh * GROUP * HD), BF),
            jax.ShapeDtypeStruct((half, rows8, HD), BF),
            jax.ShapeDtypeStruct((half, rows8, HD), BF),
        ),
        in_specs=[anywhere] * 2,
        out_specs=(anywhere,) * 3,
        scratch_shapes=[
            pltpu.VMEM((SPAN // n_kvh, n_kvh * GROUP * HD), BF),
            pltpu.VMEM((pieces, rows8, HD), BF),
            dma((n_kvh + 2,)),
            dma((n_kvh + 2,)),
        ],
        name="place_outputs",
    )(blocks, spans)
    return attn, keys.reshape(SPAN, HD), values.reshape(SPAN, HD)


def solution(mesh):
    placed = (
        P("ctx", "kvh"),
        P("ctx", "kvh"),
        P("ctx", "kvh"),
        P("ctx", "kvh"),
        P("ctx", "kvh"),
        P(),
        P("ctx"),
        P(),
    )
    return jax.shard_map(
        per_device,
        mesh=mesh,
        in_specs=placed,
        out_specs=(P(("ctx", "kvh"), None), P("ctx", "kvh"), P("ctx", "kvh")),
        check_vma=False,
    )
```

```python
import functools
import math

import jax
import jax.numpy as jnp
from jax import lax
from jax.experimental import pallas as pl
from jax.experimental.pallas import tpu as pltpu
from jax.sharding import PartitionSpec as P

MESH = pl.DeviceIdType.MESH
SPAN = 128
HD = 128
GROUP = 8
SHARD = 512
HALF = 256
LANES = 256
VROWS = 144
AHEAD = 4
PAIR_AHEAD = 1
SINGLE = 3
BF = jnp.bfloat16
F32 = jnp.float32

FIRST = (
    ((1, 1, 0, 0, 0, 0, 3), (1, 0, 0, 0, 0, 1, 0), (1, 0, 0, 1, 0, 0, 3), (1, 1, 0, 0, 0, 0, 1), (1, 1, 0, 1, 0, 0, 2), (1, 1, 0, 0, 0, 1, 1), (1, 1, 0, 1, 0, 0, 1), (1, 0, 0, 1, 0, 1, 1), (1, 0, 0, 0, 0, 0, 2), (1, 0, 0, 0, 0, 0, 1), (1, 0, 0, 1, 0, 0, 1), (1, 1, 0, 1, 0, 1, 0)),
    ((1, 1, 1, 1, 0, 0, 3), (1, 1, 1, 0, 0, 1, 1), (1, 0, 1, 1, 0, 0, 3), (1, 0, 1, 0, 0, 0, 3), (1, 1, 1, 0, 0, 0, 3)),
    ((1, 1, 2, 0, 0, 1, 3), (1, 1, 2, 1, 0, 0, 3), (1, 0, 2, 1, 0, 0, 3), (1, 1, 2, 0, 0, 0, 3), (1, 1, 2, 1, 0, 1, 3), (1, 0, 2, 0, 0, 0, 3), (1, 0, 2, 1, 0, 1, 3), (1, 0, 2, 0, 0, 1, 3)),
    ((1, 0, 3, 1, 0, 0, 1), (1, 0, 3, 0, 0, 0, 1), (1, 1, 3, 0, 0, 1, 3), (1, 1, 3, 1, 0, 0, 1)),
)
SEQ = (
    (
        ((2, 0), (0, 0, 0, 0, 1), (1, 0, 0, 0, 1, 0, 2), (1, 0, 0, 0, 1, 0, 1), (2, 1), (5, 0), (2, 2), (3,), (0, 1, 0, 1, 1), (1, 1, 0, 1, 1, 0, 1), (0, 1, 0, 0, 1), (0, 0, 0, 1, 1)),
        ((0, 0, 3, 1, 1), (0, 1, 3, 0, 1), (0, 0, 3, 0, 1), (0, 1, 3, 1, 1)),
        ((0, 1, 2, 0, 1), (0, 1, 2, 1, 1), (5, 1), (0, 0, 2, 1, 1), (0, 0, 2, 0, 1)),
        ((0, 0, 3, 1, 2), (0, 0, 3, 0, 2), (0, 1, 3, 0, 2), (0, 1, 3, 1, 2)),
        ((0, 1, 1, 0, 1), (0, 1, 1, 1, 1), (0, 0, 1, 1, 1), (0, 0, 1, 0, 1)),
        ((0, 1, 2, 0, 2), (0, 1, 2, 1, 2), (0, 0, 2, 1, 2), (0, 0, 2, 0, 2)),
        ((0, 0, 1, 1, 2), (0, 1, 1, 1, 2), (0, 0, 1, 0, 2), (0, 1, 1, 0, 2)),
    ),
    (
        ((0, 1, 0, 0, 0), (0, 1, 0, 1, 0), (0, 0, 0, 0, 0), (0, 0, 0, 1, 0)),
        ((2, 0), (0, 1, 1, 0, 1), (1, 1, 1, 0, 1, 0, 3), (1, 1, 1, 0, 1, 0, 0), (0, 0, 3, 1, 0), (1, 0, 3, 1, 0, 1, 1), (0, 0, 3, 0, 0), (1, 0, 3, 0, 0, 1, 1), (0, 1, 0, 0, 1), (1, 1, 0, 0, 1, 0, 0), (1, 1, 0, 0, 1, 0, 3), (2, 1), (0, 1, 3, 1, 0), (1, 1, 3, 1, 0, 1, 1), (5, 0), (0, 0, 0, 1, 1), (1, 0, 0, 1, 1, 0, 0), (0, 0, 3, 1, 1), (1, 0, 3, 1, 1, 1, 1), (1, 0, 3, 1, 1, 0, 3), (1, 0, 3, 1, 1, 0, 0), (0, 1, 3, 0, 1), (1, 1, 3, 0, 1, 0, 0), (2, 2), (3,), (0, 0, 3, 0, 1), (1, 0, 3, 0, 1, 0, 3), (1, 0, 3, 0, 1, 1, 1), (1, 0, 3, 0, 1, 0, 0), (0, 1, 2, 0, 1), (1, 1, 2, 0, 1, 0, 0), (1, 1, 2, 0, 1, 1, 1), (0, 1, 3, 1, 1), (1, 1, 3, 1, 1, 1, 1), (1, 1, 3, 1, 1, 0, 3), (1, 1, 3, 1, 1, 0, 0), (0, 1, 2, 1, 1), (1, 1, 2, 1, 1, 0, 0), (1, 1, 2, 1, 1, 1, 1)),
        ((0, 0, 3, 1, 2), (1, 0, 3, 1, 2, 0, 2), (1, 0, 3, 1, 2, 0, 0), (0, 0, 2, 1, 1), (1, 0, 2, 1, 1, 1, 1), (1, 0, 2, 1, 1, 0, 0), (0, 0, 0, 0, 1), (0, 1, 0, 1, 1)),
        ((0, 0, 3, 0, 2), (1, 0, 3, 0, 2, 0, 0), (0, 1, 3, 0, 2), (1, 1, 3, 0, 2, 0, 0), (5, 1), (0, 1, 2, 0, 2), (1, 1, 2, 0, 2, 0, 0), (0, 0, 2, 0, 1), (1, 0, 2, 0, 1, 0, 0), (1, 0, 2, 0, 1, 1, 1)),
        ((0, 1, 3, 1, 2), (1, 1, 3, 1, 2, 0, 2), (1, 1, 3, 1, 2, 0, 0), (0, 1, 1, 1, 1), (1, 1, 1, 1, 1, 0, 0), (1, 1, 1, 1, 1, 1, 0)),
        ((0, 1, 2, 1, 2), (1, 1, 2, 1, 2, 0, 0), (0, 0, 1, 1, 1), (1, 0, 1, 1, 1, 0, 0), (0, 0, 2, 1, 2), (1, 0, 2, 1, 2, 0, 0), (0, 0, 1, 0, 1), (1, 0, 1, 0, 1, 0, 0), (1, 0, 1, 0, 1, 1, 0)),
        ((0, 0, 2, 0, 2), (1, 0, 2, 0, 2, 0, 0)),
    ),
    (
        ((2, 0), (2, 1), (5, 0), (2, 2), (3,), (0, 1, 0, 1, 0), (1, 1, 0, 1, 0, 0, 3), (1, 1, 0, 1, 0, 1, 2), (0, 1, 2, 0, 1), (0, 1, 2, 1, 1), (0, 0, 2, 1, 1), (0, 0, 2, 0, 1)),
        ((0, 0, 0, 0, 0), (1, 0, 0, 0, 0, 0, 3), (0, 1, 0, 0, 0), (0, 0, 0, 1, 0)),
        ((0, 1, 1, 1, 0), (0, 0, 1, 1, 0), (0, 0, 1, 0, 0), (5, 1), (0, 1, 1, 0, 0)),
        ((0, 0, 0, 0, 1), (1, 0, 0, 0, 1, 0, 3), (0, 1, 1, 1, 1), (0, 0, 1, 1, 1), (0, 0, 1, 0, 1), (0, 1, 1, 0, 1)),
        ((0, 1, 0, 1, 1), (1, 1, 0, 1, 1, 0, 3), (0, 0, 0, 1, 1), (0, 1, 0, 0, 1)),
        ((0, 1, 3, 0, 1), (0, 0, 3, 1, 1), (0, 0, 3, 0, 1), (0, 1, 3, 1, 1)),
        ((0, 1, 3, 0, 2), (0, 0, 3, 1, 2), (0, 0, 3, 0, 2), (0, 1, 3, 1, 2)),
    ),
    (
        ((0, 1, 2, 1, 0), (0, 0, 2, 1, 0), (0, 1, 2, 0, 0), (0, 0, 2, 0, 0)),
        ((2, 0), (0, 1, 3, 0, 1), (1, 1, 3, 0, 1, 1, 3), (1, 1, 3, 0, 1, 0, 1), (1, 1, 3, 0, 1, 0, 2), (0, 1, 2, 0, 1), (1, 1, 2, 0, 1, 0, 2), (1, 1, 2, 0, 1, 0, 1), (0, 1, 1, 1, 0), (1, 1, 1, 1, 0, 1, 3), (1, 1, 1, 1, 0, 0, 2), (0, 1, 2, 1, 1), (1, 1, 2, 1, 1, 0, 1), (1, 1, 2, 1, 1, 0, 2), (2, 1), (0, 1, 0, 0, 0), (1, 1, 0, 0, 0, 0, 2), (5, 0), (0, 0, 2, 1, 1), (1, 0, 2, 1, 1, 0, 1), (1, 0, 2, 1, 1, 0, 2), (0, 0, 1, 1, 0), (1, 0, 1, 1, 0, 1, 3), (1, 0, 1, 1, 0, 0, 2), (0, 0, 0, 1, 0), (1, 0, 0, 1, 0, 0, 2), (1, 0, 0, 1, 0, 1, 3), (0, 1, 3, 0, 2), (1, 1, 3, 0, 2, 0, 1), (1, 1, 3, 0, 2, 0, 2), (2, 2), (3,), (0, 0, 2, 0, 1), (1, 0, 2, 0, 1, 0, 1), (1, 0, 2, 0, 1, 0, 2), (0, 1, 1, 1, 1), (1, 1, 1, 1, 1, 0, 2), (1, 1, 1, 1, 1, 0, 1), (0, 0, 1, 0, 0), (1, 0, 1, 0, 0, 0, 2), (1, 0, 1, 0, 0, 1, 3)),
        ((0, 0, 1, 1, 1), (1, 0, 1, 1, 1, 0, 1), (1, 0, 1, 1, 1, 1, 3), (1, 0, 1, 1, 1, 0, 2), (0, 0, 0, 1, 1), (1, 0, 0, 1, 1, 0, 2), (0, 1, 1, 0, 0), (1, 1, 1, 0, 0, 0, 2)),
        ((0, 0, 1, 0, 1), (1, 0, 1, 0, 1, 0, 1), (1, 0, 1, 0, 1, 0, 2), (5, 1), (0, 1, 1, 0, 1), (1, 1, 1, 0, 1, 1, 3), (1, 1, 1, 0, 1, 0, 2)),
        ((0, 0, 1, 1, 2), (1, 0, 1, 1, 2, 0, 0), (0, 1, 0, 0, 1), (1, 1, 0, 0, 1, 0, 2), (0, 1, 0, 1, 0), (0, 0, 0, 0, 0)),
        ((0, 0, 3, 1, 1), (1, 0, 3, 1, 1, 0, 2), (0, 1, 1, 0, 2), (1, 1, 1, 0, 2, 0, 0), (0, 0, 3, 0, 1), (1, 0, 3, 0, 1, 0, 2), (1, 0, 3, 0, 1, 1, 2), (0, 1, 3, 1, 1), (1, 1, 3, 1, 1, 0, 2)),
        ((0, 0, 0, 0, 1), (0, 1, 0, 1, 1)),
    ),
)
STAGE_TWO = 5
ORDER = ((4, 7, 6, 11, 5, 10, 9), (0, 7, 4, 6, 11, 5, 10), (6, 0, 1, 5, 4, 7, 11), (2, 6, 1, 5, 0, 7, 4))


def slot_of(age, home):
    return age * 4 + home


def per_device(
    queries, cache_keys, cache_values, new_keys, new_values, cache_fill, span_pos, destination
):
    n_ctx = lax.axis_size("ctx")
    n_kvh = lax.axis_size("kvh")
    planes = n_ctx // 4
    pieces = n_ctx
    scaling = HD ** (-0.5) * math.log2(math.e)

    def kernel(
        q_hbm, ck_hbm, cv_hbm, nk_hbm, nv_hbm, fill_hbm, pos_hbm, dest_hbm,
        arecv, app,
        q_ref, ck_ref, cv_ref, fill_ref, pos_ref, dest_ref, inverse,
        qt_ref, kb, vb, nvt, acc, m_ref, obuf, pk, w1, w2,
        load, ss, rs, a_s, a_r, w_s, w_r, home, spread, across,
    ):
        me = lax.axis_index("ctx")
        head = lax.axis_index("kvh")
        plane = me // 4
        role = lax.rem(me, 4)

        def at(up, r):
            return (lax.rem(plane + up + planes, planes) * 4 + r, head)

        barrier = pltpu.get_barrier_semaphore()
        near = [at(0, role ^ 1), at(0, role ^ 2), at(0, role ^ 3)]
        near += [at(1, role), at(-1, role), at(1, role ^ 1), at(-1, role ^ 1)]
        beside = [(me, lax.rem(head + 2, n_kvh)), (me, lax.rem(head + n_kvh - 2, n_kvh)), (me, head ^ 1)]
        near += beside
        for device in near:
            pl.semaphore_signal(barrier, inc=1, device_id=device, device_id_type=MESH)

        half = pieces // 2
        loads = [
            pltpu.make_async_copy(src, dst, load.at[i])
            for i, (src, dst) in enumerate((
                (fill_hbm, fill_ref), (ck_hbm, ck_ref), (cv_hbm, cv_ref), (dest_hbm, dest_ref),
                (nk_hbm, pk.at[pl.ds(0, half)]), (nv_hbm, pk.at[pl.ds(half, half)]),
                (q_hbm, q_ref), (pos_hbm, pos_ref),
            ))
        ]
        for copy in loads:
            copy.start()
        for copy in loads[:3]:
            copy.wait()

        own = role
        live = fill_ref[me]
        keys = ck_ref[...].astype(F32)
        alive = lax.broadcasted_iota(jnp.int32, (SHARD, HD), 0) < live
        keys = jnp.where(alive, keys, keys[0:1, :]).astype(BF)
        values = jnp.where(alive, cv_ref[...].astype(F32), 0.0)
        for c in range(2):
            kb[own * 2 + c] = keys[c * HALF:(c + 1) * HALF]
            vb[own * 2 + c, 0:HD, :] = values[c * HALF:(c + 1) * HALF].T.astype(BF)

        for copy in loads[3:]:
            copy.wait()

        pl.semaphore_wait(barrier, len(near))

        def piece(t, j, c, age):
            if t == 0:
                return kb.at[slot_of(age, j) * 2 + c]
            return vb.at[slot_of(age, j) * 2 + c, pl.ds(0, HD)]

        def remote(t, j, c, age, up, r):
            return pltpu.make_async_remote_copy(
                src_ref=piece(t, j, c, age),
                dst_ref=piece(t, j, c, age + up),
                send_sem=ss.at[t],
                recv_sem=rs.at[t, slot_of(age + up, j), c],
                device_id=at(up, r),
                device_id_type=MESH,
            )

        def act(action):
            if action[0] == 0:
                _, t, j, c, age = action
                pltpu.make_async_remote_copy(
                    src_ref=piece(t, j, c, age),
                    dst_ref=piece(t, j, c, age),
                    send_sem=ss.at[t],
                    recv_sem=rs.at[t, slot_of(age, j), c],
                    device_id=at(0, role ^ 1),
                    device_id_type=MESH,
                ).wait_recv()
            elif action[0] == 2:
                spread_round(action[1])
            elif action[0] == 5:
                pl.semaphore_wait(across.at[action[1]], 3)
                if action[1] == 0:
                    signal_beside(1)
            elif action[0] == 3:
                stage_one()
            else:
                remote(*action[1:]).start()

        for r in range(4):
            @pl.when(role == r)
            def _(r=r):
                for action in FIRST[r]:
                    act(action)

        def signal_planes(k, step):
            for up in (step, -step):
                pl.semaphore_signal(spread.at[k], inc=1, device_id=at(up, role), device_id_type=MESH)

        def signal_beside(k):
            for device in beside:
                pl.semaphore_signal(across.at[k], inc=1, device_id=device, device_id_type=MESH)

        signal_planes(0, 1)
        signal_beside(0)

        @pl.loop(0, n_ctx)
        def _(d):
            source = jnp.int32(0)
            for g in range(n_ctx):
                source = jnp.maximum(source, jnp.where(dest_ref[g] == d, g, 0))
            inverse[d] = source

        for b in range(SPAN // 16):
            rows = [q_ref[b * 16:(b + 1) * 16, g * HD:(g + 1) * HD] for g in range(GROUP)]
            block = jnp.concatenate(rows, axis=0)
            qt_ref[:, b * 128:(b + 1) * 128] = block.astype(F32).T.astype(BF)
        row16 = lax.broadcasted_iota(jnp.int32, (16, HALF), 0)
        lane16 = lax.broadcasted_iota(jnp.int32, (16, HALF), 1)
        nvt[0:HD, :] = pk[half:pieces].reshape(SPAN, HD).astype(F32).T.astype(BF)
        nvt[HD:VROWS, :] = jnp.where(row16[:, :SPAN] == 0, 1.0, 0.0).astype(BF)
        for age in range(3):
            for j in range(4):
                filled = fill_ref[at(-age, j)[0]]
                for c in range(2):
                    seen = (row16 == 0) & (lane16 + c * HALF < filled)
                    vb[slot_of(age, j) * 2 + c, HD:VROWS, :] = jnp.where(seen, 1.0, 0.0).astype(BF)

        def tokens(tile, rows):
            lane = lax.broadcasted_iota(jnp.int32, (rows, LANES), 1)
            return (tile * 2 + lane // 128) * 16 + lane % 16

        def dot(a, b):
            return jnp.dot(a, b, preferred_element_type=F32)

        def lanes_of(tile):
            if isinstance(tile, int):
                return pl.ds(tile * LANES, LANES)
            return pl.ds(pl.multiple_of(tile * LANES, LANES), LANES)

        tiles = (GROUP * SPAN) // LANES

        def own_scores(tile):
            s = dot(pk[0:half].reshape(SPAN, HD), qt_ref[:, lanes_of(tile)])
            row = lax.broadcasted_iota(jnp.int32, (SPAN, LANES), 0)
            return jnp.where(row <= tokens(tile, SPAN), s, -1e30)

        def own_absorb(tile, s):
            lanes = lanes_of(tile)
            top = jnp.max(s, axis=0, keepdims=True)
            weights = jnp.exp2((s - top) * scaling).astype(BF)
            acc[:, lanes] = dot(nvt[...], weights)
            m_ref[:, lanes] = top

        def shard_scores(slots, home, tile):
            qt = qt_ref[:, lanes_of(tile)]
            parts = []
            for slot in slots:
                for c in range(2):
                    s = dot(kb[slot * 2 + c], qt)
                    if home:
                        row = lax.broadcasted_iota(jnp.int32, (HALF, LANES), 0) + c * HALF
                        s = jnp.where(row <= tokens(tile, HALF) + pos_ref[0], s, -1e30)
                    parts.append(s)
            return parts

        def shard_absorb(slots, final, tile, parts):
            lanes = lanes_of(tile)
            old = m_ref[:, lanes]
            top = jnp.maximum(old, jnp.max(functools.reduce(jnp.maximum, parts), axis=0, keepdims=True))
            total = acc[:, lanes] * jnp.exp2((old - top) * scaling)
            for i, part in enumerate(parts):
                weights = jnp.exp2((part - top) * scaling).astype(BF)
                total = total + dot(vb[slots[i // 2] * 2 + i % 2], weights)
            if final:
                return total
            acc[:, lanes] = total
            m_ref[:, lanes] = top

        def in_turn(order, scores, absorb, after=None, depth=AHEAD):
            ahead = [scores(tile) for tile in order[:depth]]
            for i, tile in enumerate(order):
                if i + depth < len(order):
                    ahead.append(scores(order[i + depth]))
                total = absorb(tile, ahead.pop(0))
                if after is not None:
                    after(i, tile, total)

        def attend(slots, home=False, order=tuple(range(tiles)), after=None):
            in_turn(
                order,
                functools.partial(shard_scores, slots, home),
                functools.partial(shard_absorb, slots, after is not None),
                after,
                AHEAD if len(slots) == 1 else PAIR_AHEAD,
            )

        in_turn(tuple(range(tiles)), own_scores, own_absorb)
        attend((own,), home=True)

        def spread_round(k):
            pl.semaphore_wait(spread.at[k], 2)
            if k == 0:
                signal_planes(1, 2)
            elif k == 1:
                signal_planes(2, 1)

        def stage_copy(src, dst, stage, device):
            return pltpu.make_async_remote_copy(
                src_ref=src, dst_ref=dst, send_sem=w_s.at[stage], recv_sem=w_r.at[stage],
                device_id=(device, head), device_id_type=MESH,
            )

        def stage_wait(src, dst, stage):
            most = pl.ds(0, n_ctx - 1)
            stage_copy(src.at[most], dst.at[most], stage, me ^ 1).wait()

        def other(k):
            return lax.rem(me + k, n_ctx)

        def stage_one():
            w1[me] = pk[me]

            @pl.loop(1, n_ctx)
            def _(k):
                stage_copy(pk.at[other(k)], w1.at[me], 0, other(k)).start()

        def stage_two():
            stage_wait(pk, w1, 0)

            @pl.loop(0, n_ctx)
            def _(d):
                w2[d] = w1[inverse[d]]

            pltpu.make_async_copy(w2.at[me], app.at[me], home.at[1]).start()

            @pl.loop(1, n_ctx)
            def _(k):
                stage_copy(w2.at[other(k)], app.at[me], 1, other(k)).start()

        def communicate(step):
            for r in range(4):
                @pl.when(role == r)
                def _(r=r):
                    for i in range(7) if not isinstance(step, int) else (step,):
                        if not isinstance(step, int):
                            if i >= SINGLE:
                                continue

                            @pl.when(step == i)
                            def _(i=i):
                                for action in SEQ[r][i]:
                                    act(action)
                        else:
                            for action in SEQ[r][i]:
                                act(action)
            if isinstance(step, int) and step == STAGE_TWO:
                stage_two()

        def slot_at(step):
            slot = jnp.int32(0)
            for r in range(4):
                code = jnp.int32(ORDER[r][0])
                for i in range(1, 7):
                    code = jnp.where(step == i, ORDER[r][i], code)
                slot = jnp.where(role == r, code, slot)
            return slot

        @pl.loop(0, SINGLE)
        def _(step):
            communicate(step)
            attend((slot_at(step),))

        for step in range(SINGLE, 5, 2):
            communicate(step)
            communicate(step + 1)
            attend((slot_at(step), slot_at(step + 1)))

        communicate(5)
        communicate(6)
        last = (slot_at(5), slot_at(6))

        def out_copy(b):
            return pltpu.make_async_remote_copy(
                src_ref=obuf.at[b], dst_ref=arecv.at[head], send_sem=a_s.at[b], recv_sem=a_r.at[head],
                device_id=(me, b), device_id_type=MESH,
            )

        def ship(i):
            if i < tiles - 1:
                for part in range(2):
                    out_copy(turn[i] * 2 + part).start()
            else:
                out_copy(head ^ 1).start()
                pltpu.make_async_copy(obuf.at[head], arecv.at[head], home.at[0]).start()

        turn = [lax.rem(head // 2 + i, tiles) for i in (2, 1, 3, 0)]

        def finish(i, tile, total):
            result = total[0:HD] * (1.0 / total[HD:HD + 1])
            result = result.T.astype(BF)
            for part in range(2):
                for g in range(GROUP):
                    at_row = part * 128 + g * 16
                    obuf[tile * 2 + part, :, g * HD:(g + 1) * HD] = result[at_row:at_row + 16]
            if i > 0:
                ship(i - 1)

        attend(last, order=turn, after=finish)
        ship(tiles - 1)
        if STAGE_TWO == 7:
            stage_two()

        for r in range(4):
            @pl.when(role == r)
            def _(r=r):
                for t in range(2):
                    actions = FIRST[r] + sum(SEQ[r], ())
                    count = sum(a[:2] == (1, t) for a in actions)
                    whole = kb.at[pl.ds(0, count)] if t == 0 else vb.at[pl.ds(0, count), pl.ds(0, HD)]
                    pltpu.make_async_remote_copy(
                        src_ref=whole, dst_ref=whole, send_sem=ss.at[t], recv_sem=rs.at[0, 0, 0],
                        device_id=at(0, role ^ 1), device_id_type=MESH,
                    ).wait_send()

        for k in range(1, n_kvh):
            h = lax.rem(head + k, n_kvh)
            pltpu.make_async_remote_copy(
                src_ref=obuf.at[h], dst_ref=arecv.at[h], send_sem=a_s.at[h], recv_sem=a_r.at[h],
                device_id=(me, h), device_id_type=MESH,
            ).wait()
        stage_wait(w2, app, 1)
        pltpu.make_async_copy(obuf.at[head], arecv.at[head], home.at[0]).wait()
        pltpu.make_async_copy(w2.at[me], app.at[me], home.at[1]).wait()

    half = pieces // 2
    rows8 = SPAN // half
    dma = pltpu.SemaphoreType.DMA
    blocks, spans = pl.pallas_call(
        kernel,
        out_shape=(
            jax.ShapeDtypeStruct((n_kvh, SPAN // n_kvh, GROUP * HD), BF),
            jax.ShapeDtypeStruct((pieces, rows8, HD), BF),
        ),
        in_specs=[pl.BlockSpec(memory_space=pl.ANY)] * 6
        + [pl.BlockSpec(memory_space=pltpu.HBM), pl.BlockSpec(memory_space=pl.ANY)],
        out_specs=(pl.BlockSpec(memory_space=pl.ANY),) * 2,
        scratch_shapes=[
            pltpu.VMEM((SPAN, GROUP * HD), BF),
            pltpu.VMEM((SHARD, HD), BF),
            pltpu.VMEM((SHARD, HD), BF),
            pltpu.SMEM((n_ctx,), jnp.int32),
            pltpu.SMEM((1,), jnp.int32),
            pltpu.SMEM((n_ctx,), jnp.int32),
            pltpu.SMEM((n_ctx,), jnp.int32),
            pltpu.VMEM((HD, GROUP * SPAN), BF),
            pltpu.VMEM((32, HALF, HD), BF),
            pltpu.VMEM((32, VROWS, HALF), BF),
            pltpu.VMEM((VROWS, SPAN), BF),
            pltpu.VMEM((VROWS, GROUP * SPAN), F32),
            pltpu.VMEM((1, GROUP * SPAN), F32),
            pltpu.VMEM((n_kvh, SPAN // n_kvh, GROUP * HD), BF),
            pltpu.VMEM((pieces, rows8, HD), BF),
            pltpu.VMEM((pieces, rows8, HD), BF),
            pltpu.VMEM((pieces, rows8, HD), BF),
            dma((8,)),
            dma((2,)),
            dma((2, 12, 2)),
            dma((n_kvh,)),
            dma((n_kvh,)),
            dma((2,)),
            dma((2,)),
            dma((2,)),
            pltpu.SemaphoreType.REGULAR((3,)),
            pltpu.SemaphoreType.REGULAR((2,)),
        ],
        compiler_params=pltpu.CompilerParams(
            collective_id=0, has_side_effects=True
        ),
        name="spanned_attention",
    )(
        queries, cache_keys, cache_values,
        new_keys.reshape(half, rows8, HD), new_values.reshape(half, rows8, HD),
        cache_fill, span_pos, destination,
    )

    def place(blocks_ref, spans_ref, out_ref, ak_ref, av_ref, rows, spans_here, taken, given):
        def columns(ref, h):
            return ref.at[:, pl.ds(h * GROUP * HD, GROUP * HD)]

        moves = [
            (blocks_ref.at[h], columns(rows, h), columns(rows, h), columns(out_ref, h)) for h in range(n_kvh)
        ]
        for part, target in ((0, ak_ref), (half, av_ref)):
            some = pl.ds(part, half)
            moves.append((spans_ref.at[some], spans_here.at[some], spans_here.at[some], target))
        takes = [pltpu.make_async_copy(m[0], m[1], taken.at[i]) for i, m in enumerate(moves)]
        gives = [pltpu.make_async_copy(m[2], m[3], given.at[i]) for i, m in enumerate(moves)]
        for copy in takes:
            copy.start()
        for take, give in zip(takes, gives):
            take.wait()
            give.start()
        for copy in gives:
            copy.wait()

    anywhere = pl.BlockSpec(memory_space=pl.ANY)
    attn, keys, values = pl.pallas_call(
        place,
        out_shape=(
            jax.ShapeDtypeStruct((SPAN // n_kvh, n_kvh * GROUP * HD), BF),
            jax.ShapeDtypeStruct((half, rows8, HD), BF),
            jax.ShapeDtypeStruct((half, rows8, HD), BF),
        ),
        in_specs=[anywhere] * 2,
        out_specs=(anywhere,) * 3,
        scratch_shapes=[
            pltpu.VMEM((SPAN // n_kvh, n_kvh * GROUP * HD), BF),
            pltpu.VMEM((pieces, rows8, HD), BF),
            dma((n_kvh + 2,)),
            dma((n_kvh + 2,)),
        ],
        name="place_outputs",
    )(blocks, spans)
    return attn, keys.reshape(SPAN, HD), values.reshape(SPAN, HD)


def solution(mesh):
    placed = (
        P("ctx", "kvh"),
        P("ctx", "kvh"),
        P("ctx", "kvh"),
        P("ctx", "kvh"),
        P("ctx", "kvh"),
        P(),
        P("ctx"),
        P(),
    )
    return jax.shard_map(
        per_device,
        mesh=mesh,
        in_specs=placed,
        out_specs=(P(("ctx", "kvh"), None), P("ctx", "kvh"), P("ctx", "kvh")),
        check_vma=False,
    )
```
